256 devices in a mesh: row: 32 (over y, x, core), col: 8 (over z).
Axes of the slice: x: 4, y: 4, z: 8, core: 2. Of those that a mesh axis runs over, the one named last changes fastest.
Arguments:
- right_side: float32 [2, 8192, 2048], P(None, 'row', 'col'), may hold values from -6 to 6
- probe: float32 [2, 256, 256], replicated, may hold values from -6 to 6
- detector_weights: float32 [256, 256], replicated, may hold values from 0.1 to 10
- offsets: int32 [32, 8, 4, 2], P('row', 'col'), may hold values from -128 to 127, as said below
- counts: int32 [32, 8], P('row', 'col'), may hold values from 2 to 4, as said below
Outputs:
- solution_field: float32 [2, 8192, 2048], P(None, 'row', 'col')
- residual: float32 [2, 8192, 2048], P(None, 'row', 'col')
The draws below stay inside these ranges and needn't reach their ends.
Inputs may be any that keep to these rules, and one draw needn't show every extreme that they name: `counts`: every region holds at least two positions; in every draw some region holds exactly 4. In every region slot 0 has both offsets negative and slot 1 both offsets non-negative.
All inputs are finite; a program needn't handle non-finite values.
Results may differ from the reference program's by a relative error of at most 0.0003.
Values sent between devices are 32-bit elements; how exact they have to be, the bound alone decides.
A program may use at most 64 MiB of HBM per device.

```python
import math
import jax
import jax.numpy as jnp
from jax import lax

PATCH = 256
CAP = 4
ITERS = 3
NY = 8192
NX = 2048
N_ROW = 32
N_COL = 8


def draw_counts(key, part):
    key_full, key_low, key_pick = jax.random.split(jax.random.fold_in(key, 71), 3)
    heavy = jax.random.randint(key_full, (N_ROW, N_COL), 0, 4) == 0
    light = jax.random.randint(key_low, (N_ROW, N_COL), 2, max(CAP // 2, 2) + 1)
    filled = jnp.where(heavy, CAP, light).reshape(-1)
    chosen = jax.random.randint(key_pick, (), 0, N_ROW * N_COL)
    filled = filled.at[chosen].set(CAP)
    return filled.reshape(N_ROW, N_COL).astype(jnp.int32)


def draw_offsets(key, part):
    half = PATCH // 2
    key_rest, key_low, key_high = jax.random.split(jax.random.fold_in(key, 53), 3)
    rest = jax.random.randint(key_rest, (N_ROW, N_COL, CAP, 2), -half, half)
    low = jax.random.randint(key_low, (N_ROW, N_COL, 1, 2), -half, 0)
    high = jax.random.randint(key_high, (N_ROW, N_COL, 1, 2), 0, half)
    return jnp.concatenate([low, high, rest[:, :, 2:]], axis=2).astype(jnp.int32)


def shard_levels(stream_key, extent, shards, least, high):
    def one(position, blocks):
        draws = jax.random.uniform(jax.random.fold_in(jax.random.fold_in(stream_key, 6), position), (blocks,), jnp.float32, least / len(shards), high / len(shards))
        return jnp.repeat(jnp.exp(draws), extent[position] // blocks).reshape((-1,) + (1,) * (len(extent) - position - 1))

    gain = one(*shards[0])
    for cut in shards[1:]:
        gain = gain * one(*cut)
    return gain


def centred(own_key, shape, spread, bound, cuts=(), held_as=jnp.bfloat16):
    drawn = jax.random.normal(own_key, shape, jnp.float32) * spread
    if len(cuts) > 0:
        drawn = shard_levels(own_key, shape, cuts, -0.22, 0.18) * drawn
    return jnp.clip(drawn, min=-bound, max=bound).astype(held_as)


def setup_inputs(seed: int = 0) -> dict:
    arg_keys = jax.random.split(jax.random.key(seed), 6)
    return {
        "right_side": centred(arg_keys[0], (2, NY, NX), 1.0, 6.0, ((1, 32), (2, 8)), jnp.float32),
        "probe": centred(arg_keys[1], (2, PATCH, PATCH), 1.0, 6.0, (), jnp.float32),
        "detector_weights": jnp.clip(jnp.exp(jax.random.uniform(arg_keys[2], (PATCH, PATCH), jnp.float32, math.log(0.1), math.log(10.0))), 0.1, 10.0),
        "offsets": draw_offsets(jax.random.fold_in(arg_keys[5], 71), 0),
        "counts": draw_counts(jax.random.fold_in(arg_keys[5], 71), 0),
    }


ridge_weight = 0.5


def patch_normal(tile_in, probe, weights):
    illum = lax.complex(probe[0], probe[1])
    wave = illum * lax.complex(tile_in[0], tile_in[1])
    freq = jnp.fft.fft2(wave, norm="ortho")
    back = jnp.fft.ifft2(freq * weights, norm="ortho")
    result = jnp.conj(illum) * back
    return jnp.stack([jnp.real(result), jnp.imag(result)])


def operate(field, probe, weights, row_starts, col_starts, weight_on):
    margin = PATCH // 2
    padded = jnp.pad(field, ((0, 0), (margin, margin), (margin, margin)))

    def visit(summed, item):
        row_at, col_at, flag = item
        zero_idx = jnp.zeros((), jnp.int32)
        tile_in = lax.dynamic_slice(padded, (zero_idx, row_at, col_at), (2, PATCH, PATCH))
        update = patch_normal(tile_in, probe, weights) * flag
        current = lax.dynamic_slice(summed, (zero_idx, row_at, col_at), (2, PATCH, PATCH))
        return lax.dynamic_update_slice(summed, current + update, (zero_idx, row_at, col_at)), None

    summed, _ = lax.scan(visit, jnp.zeros_like(padded), (row_starts, col_starts, weight_on))
    return summed[:, margin:margin + NY, margin:margin + NX] + ridge_weight * field


def inner(first, second):
    return jnp.sum(first * second)


def reference(right_side, probe, detector_weights, offsets, counts):
    margin = PATCH // 2
    region_row = (jnp.arange(N_ROW, dtype=jnp.int32) * PATCH + margin)[:, None, None]
    region_col = (jnp.arange(N_COL, dtype=jnp.int32) * PATCH + margin)[None, :, None]
    row_starts = (offsets[:, :, :, 0].astype(jnp.int32) + region_row).reshape(-1).astype(jnp.int32)
    col_starts = (offsets[:, :, :, 1].astype(jnp.int32) + region_col).reshape(-1).astype(jnp.int32)
    slot_ids = jnp.arange(CAP, dtype=jnp.int32)[None, None, :]
    weight_on = (slot_ids < counts[:, :, None]).astype(jnp.float32).reshape(-1)
    solution_field = jnp.zeros_like(right_side)
    residual, direction = right_side, right_side
    norm_now = inner(residual, residual)
    for iteration in range(ITERS):
        image = operate(direction, probe, detector_weights, row_starts, col_starts, weight_on)
        alpha = norm_now / inner(direction, image)
        solution_field = solution_field + alpha * direction
        residual = residual - alpha * image
        norm_next = inner(residual, residual)
        direction = residual + (norm_next / norm_now) * direction
        norm_now = norm_next
    return solution_field, residual
```

```python
import functools
import math

import jax
import jax.numpy as jnp
import numpy as np
from jax import lax
from jax.experimental import pallas as pl
from jax.experimental.pallas import tpu as pltpu
from jax.sharding import PartitionSpec as P

ITERS = 3
ridge_weight = 0.5
MESH = pl.DeviceIdType.MESH
f32 = jnp.float32
bf16 = jnp.bfloat16


def tables(side):
    half = side // 2
    n = np.arange(half)
    found = []
    for odd in (0, 1):
        phase = ((2 * np.arange(half) + odd)[:, None] * n[None, :]) % side
        angle = phase * (-2.0 * math.pi / side)
        re, im = np.cos(angle) / math.sqrt(side), np.sin(angle) / math.sqrt(side)
        found.append(np.block([[re, -im], [im, re]]).astype(np.float32))
    full = found + [mat.T.copy() for mat in found]
    out = []
    for mat in full:
        hi = mat.astype(jnp.bfloat16)
        out += [hi, (mat - hi.astype(np.float32)).astype(jnp.bfloat16)]
    return np.stack(out)


def split(value):
    hi = value.astype(bf16)
    return hi, (value - hi.astype(f32)).astype(bf16)


def dot(left, right):
    return jnp.dot(left, right, preferred_element_type=f32)


def dot3(left, right):
    return dot(left[0], right[0]) + (dot(left[0], right[1]) + dot(left[1], right[0]))


def kernel(n_row, n_col, cap, right_ref, probe_ref, weights_ref, mats_ref, offs_ref, count_ref,
           x_out, r_out,
           field, halo_r, halo_c, halo_x, acc_o, acc_r, acc_c, acc_x, back_r, back_c, back_x,
           illum, spec_hi, spec_lo, wave_hi, wave_lo, wgt, x_ref, d_ref, along_ref, quad_ref,
           scal_ref, msg1, msg2, gs, gr, bs, br, as_, ar):
    side = field.shape[1]
    half = side // 2
    row, col = lax.axis_index("row"), lax.axis_index("col")
    odd = lax.rem(row, 2)
    near = row + 1 - 2 * odd
    far = row - 1 + 2 * odd
    has_far = jnp.logical_and(far >= 0, far < n_row)
    has_left, has_right = col > 0, col < n_col - 1
    h_far = pl.multiple_of(odd * half, half)
    h_near = pl.multiple_of(half - odd * half, half)

    for ref in (halo_r, halo_c, halo_x, back_r, back_c, back_x, x_ref, d_ref, along_ref):
        ref[...] = jnp.zeros_like(ref)
    field[...] = right_ref[...]

    barrier = pltpu.get_barrier_semaphore()

    def greet_row(step, carry):
        pl.semaphore_signal(barrier, inc=1, device_id={"row": lax.rem(row + step, n_row)}, device_id_type=MESH)
        return carry

    def greet_col(step, carry):
        pl.semaphore_signal(barrier, inc=1, device_id={"col": lax.rem(col + step, n_col)}, device_id_type=MESH)
        return carry

    lax.fori_loop(1, n_row, greet_row, 0)
    lax.fori_loop(1, n_col, greet_col, 0)
    pl.semaphore_wait(barrier, n_row + n_col - 2)

    def remote(src, dst, sems, rsems, i, target):
        return pltpu.make_async_remote_copy(
            src_ref=src, dst_ref=dst, send_sem=sems.at[i], recv_sem=rsems.at[i],
            device_id=target, device_id_type=MESH)

    def rows_of(ref, start):
        return ref.at[:, pl.ds(start, half), :]

    def block_of(ref, start, col_start):
        return ref.at[:, pl.ds(start, half), pl.ds(col_start, half)]

    def gather_copies():
        left, right = {"col": col - 1}, {"col": col + 1}
        to_left = [remote(block_of(field, h, 0), block_of(halo_c, h, 0), gs, gr, i, left)
                   for i, h in enumerate((h_far, h_near))]
        to_right = [remote(block_of(field, h, half), block_of(halo_c, h, half), gs, gr, 2 + i, right)
                    for i, h in enumerate((h_far, h_near))]
        own_far = remote(rows_of(field, h_far), rows_of(halo_r, h_far), gs, gr, 4, {"row": far})
        own_near = remote(rows_of(field, h_near), rows_of(halo_r, h_near), gs, gr, 5, {"row": near})
        cor_far = remote(rows_of(halo_c, h_far), rows_of(halo_x, h_far), gs, gr, 6, {"row": far})
        cor_near = remote(rows_of(halo_c, h_near), rows_of(halo_x, h_near), gs, gr, 7, {"row": near})
        return to_left, to_right, own_far, own_near, cor_far, cor_near

    def gather(between):
        to_left, to_right, own_far, own_near, cor_far, cor_near = gather_copies()
        for i in (0, 1):
            pl.when(has_left)(to_left[i].start)
            pl.when(has_right)(to_right[i].start)
            if i == 0:
                pl.when(has_far)(own_far.start)
                own_near.start()
        between()
        pl.when(has_right)(to_left[0].wait_recv)
        pl.when(has_left)(to_right[0].wait_recv)
        pl.when(has_far)(cor_far.start)
        pl.when(has_right)(to_left[1].wait_recv)
        pl.when(has_left)(to_right[1].wait_recv)
        cor_near.start()
        pl.when(has_far)(own_far.wait_recv)
        own_near.wait_recv()
        cor_near.wait_recv()
        pl.when(has_far)(cor_far.wait_recv)

    def gather_done():
        to_left, to_right, own_far, own_near, cor_far, cor_near = gather_copies()
        for i in (0, 1):
            pl.when(has_left)(to_left[i].wait_send)
            pl.when(has_right)(to_right[i].wait_send)
        pl.when(has_far)(own_far.wait_send)
        own_near.wait_send()
        pl.when(has_far)(cor_far.wait_send)
        cor_near.wait_send()

    def prepare():
        ramp_i = lax.broadcasted_iota(jnp.int32, (side, side), 0)
        ramp_j = lax.broadcasted_iota(jnp.int32, (side, side), 1)
        take = jnp.where(ramp_i < half, 2 * ramp_i, 2 * ramp_i + 1 - side)
        left = jnp.where(take == ramp_j, 1.0, 0.0).astype(f32)
        take_t = jnp.where(ramp_j < half, 2 * ramp_j, 2 * ramp_j + 1 - side)
        right = jnp.where(take_t == ramp_i, 1.0, 0.0).astype(f32)
        moved = jnp.dot(left, weights_ref[...], precision=lax.Precision.HIGHEST, preferred_element_type=f32)
        wgt[...] = jnp.dot(moved, right, precision=lax.Precision.HIGHEST, preferred_element_type=f32)

        def place(s, carry):
            down, across = offs_ref[s, 0], offs_ref[s, 1]
            down = jnp.where(down < 0, down + side, down)
            across = jnp.where(across < 0, across + side, across)
            flag = jnp.where(s < count_ref[0, 0], 1.0, 0.0).astype(f32)
            for part in (0, 1):
                rolled = pltpu.roll(probe_ref[part] * flag, down, 0)
                illum[s, part] = pltpu.roll(rolled, across, 1)
            return carry

        lax.fori_loop(0, cap, place, 0)
        scal_ref[0] = jnp.ones_like(scal_ref[0])
        scal_ref[1] = jnp.ones_like(scal_ref[1])
        first = field[...]
        scal_ref[2, 0:1, :] = lanes(jnp.sum(first * first, axis=(0, 1))[None])

    def lanes(value):
        return value[:, :half] + value[:, half:]

    def masks(s, h):
        down, across = offs_ref[s, 0], offs_ref[s, 1]
        t = lax.broadcasted_iota(jnp.int32, (half, half), 0) + h * half
        u = lax.broadcasted_iota(jnp.int32, (half, half), 1)
        row_in = jnp.logical_and(t >= down, t < down + side)
        col_in = (u >= across, u + half < across + side)
        return row_in, col_in

    def forward(s, carry):
        found = []
        for h in (0, 1):
            rows = slice(h * half, (h + 1) * half)
            row_in, col_in = masks(s, h)
            view = []
            for part in (0, 1):
                pieces = []
                for j in (0, 1):
                    cols = slice(j * half, (j + 1) * half)
                    inner = jnp.where(row_in, field[part, rows, cols], halo_r[part, rows, cols])
                    outer = jnp.where(row_in, halo_c[part, rows, cols], halo_x[part, rows, cols])
                    pieces.append(jnp.where(col_in[j], inner, outer))
                view.append(pieces)
            wave = []
            for j in (0, 1):
                cols = slice(j * half, (j + 1) * half)
                pr, pi = illum[s, 0, rows, cols], illum[s, 1, rows, cols]
                vr, vi = view[0][j], view[1][j]
                wave.append((pr * vr - pi * vi, pr * vi + pi * vr))
            plus = jnp.concatenate([wave[0][0] + wave[1][0], wave[0][1] + wave[1][1]], axis=1)
            minus = jnp.concatenate([wave[0][0] - wave[1][0], wave[0][1] - wave[1][1]], axis=1)
            found.append((
                dot3(split(plus), (mats_ref[4], mats_ref[5])),
                dot3(split(minus), (mats_ref[6], mats_ref[7])),
            ))
        quad = jnp.zeros((1, side), f32)
        for which, sign in ((0, 1.0), (1, -1.0)):
            both = [found[0][j] + sign * found[1][j] for j in (0, 1)]
            stacked = jnp.concatenate([
                jnp.concatenate([both[0][:, :half], both[1][:, :half]], axis=1),
                jnp.concatenate([both[0][:, half:], both[1][:, half:]], axis=1)], axis=0)
            freq = dot3((mats_ref[2 * which], mats_ref[2 * which + 1]), split(stacked))
            scale = wgt[which * half:(which + 1) * half, :]
            scaled = freq * jnp.concatenate([scale, scale], axis=0)
            quad = quad + jnp.sum(freq * scaled, axis=0, keepdims=True)
            hi, lo = split(scaled)
            spec_hi[s, which] = hi
            spec_lo[s, which] = lo
        quad_ref[...] += lanes(quad)
        return carry

    def inverse(s, carry):
        even = dot3((mats_ref[4], mats_ref[5]), (spec_hi[s, 0], spec_lo[s, 0]))
        odd_ = dot3((mats_ref[6], mats_ref[7]), (spec_hi[s, 1], spec_lo[s, 1]))
        for h in (0, 1):
            rows = slice(h * half, (h + 1) * half)
            both = even + odd_ if h == 0 else even - odd_
            out = []
            for j in (0, 1):
                cols = slice(j * half, (j + 1) * half)
                lhs = jnp.concatenate([both[:half, cols], both[half:, cols]], axis=1)
                out.append(dot3(split(lhs), (mats_ref[2 * j], mats_ref[2 * j + 1])))
            row_in, col_in = masks(s, h)
            for j in (0, 1):
                cols = slice(j * half, (j + 1) * half)
                mixed = out[0] + out[1] if j == 0 else out[0] - out[1]
                hr, hi = mixed[:, :half], mixed[:, half:]
                pr, pi = illum[s, 0, rows, cols], illum[s, 1, rows, cols]
                for part, term in ((0, pr * hr + pi * hi), (1, pr * hi - pi * hr)):
                    inner = jnp.where(row_in, term, 0.0)
                    outer = term - inner
                    inner_own = jnp.where(col_in[j], inner, 0.0)
                    outer_own = jnp.where(col_in[j], outer, 0.0)
                    acc_o[part, rows, cols] += inner_own
                    acc_c[part, rows, cols] += inner - inner_own
                    acc_r[part, rows, cols] += outer_own
                    acc_x[part, rows, cols] += outer - outer_own
        return carry

    def share(msg, mine, k, count, axis, at, i):
        def send(step, carry):
            remote_to = {axis: lax.rem(mine + step, count)}
            pltpu.make_async_remote_copy(
                src_ref=msg.at[k, mine], dst_ref=msg.at[k, mine], send_sem=as_.at[i, k], recv_sem=ar.at[i, k],
                device_id=remote_to, device_id_type=MESH).start()
            return carry
        msg[k, at] = scal_ref[2]
        lax.fori_loop(1, count, send, 0)

    def shared(msg, k, count, sem, i):
        part = msg.at[k, pl.ds(0, count - 1)]
        pltpu.make_async_copy(part, part, sem.at[i, k]).wait()

    def back_copies():
        left, right = {"col": col - 1}, {"col": col + 1}
        cor_near = remote(rows_of(acc_x, h_far), rows_of(back_x, h_far), bs, br, 0, {"row": near})
        cor_far = remote(rows_of(acc_x, h_near), rows_of(back_x, h_near), bs, br, 1, {"row": far})
        own_near = remote(rows_of(acc_r, h_far), rows_of(back_r, h_far), bs, br, 2, {"row": near})
        own_far = remote(rows_of(acc_r, h_near), rows_of(back_r, h_near), bs, br, 3, {"row": far})
        to_right = [remote(block_of(acc_c, h, 0), block_of(back_c, h, 0), bs, br, 4 + i, right)
                    for i, h in enumerate((h_near, h_far))]
        to_left = [remote(block_of(acc_c, h, half), block_of(back_c, h, half), bs, br, 6 + i, left)
                   for i, h in enumerate((h_near, h_far))]
        return cor_near, cor_far, own_near, own_far, to_right, to_left

    def iteration(k, carry):
        gather(lambda: pl.when(k == 0)(prepare))
        quad_ref[...] = jnp.zeros_like(quad_ref)
        lax.fori_loop(0, cap, forward, 0)
        scal_ref[2, 1:2, :] = quad_ref[...] + ridge_weight * scal_ref[2, 0:1, :]
        share(msg1, row, k, n_row, "row", row, 0)
        gather_done()
        acc_o[...] = ridge_weight * field[...]
        for ref in (acc_r, acc_c, acc_x):
            ref[...] = jnp.zeros_like(ref)
        lax.fori_loop(0, cap, inverse, 0)

        cor_near, cor_far, own_near, own_far, to_right, to_left = back_copies()
        cor_near.start()
        pl.when(has_far)(cor_far.start)
        own_near.start()
        pl.when(has_far)(own_far.start)
        shared(msg1, k, n_row, ar, 0)
        scal_ref[2] = jnp.sum(msg1[k], axis=0)
        share(msg2, col, k, n_col, "col", col, 1)
        cor_near.wait_recv()
        for i, h in ((0, h_near), (1, h_far)):
            if i == 1:
                pl.when(has_far)(cor_far.wait_recv)
            acc_c[:, pl.ds(h, half), :] += back_x[:, pl.ds(h, half), :]
            pl.when(has_right)(to_right[i].start)
            pl.when(has_left)(to_left[i].start)
        shared(msg2, k, n_col, ar, 1)
        total = jnp.sum(jnp.sum(msg2[k], axis=0), axis=1, keepdims=True)
        norm, product = total[0:1], total[1:2]
        before, alpha_before = scal_ref[0, 0:1, 0:1], scal_ref[1, 0:1, 0:1]
        ratio = jnp.where(k == 0, jnp.zeros_like(norm), norm / before)
        alpha = norm / (product - ratio * norm / alpha_before)
        scal_ref[0] = jnp.broadcast_to(norm, scal_ref.shape[1:])
        scal_ref[1] = jnp.broadcast_to(alpha, scal_ref.shape[1:])
        own_near.wait_recv()
        pl.when(has_far)(own_far.wait_recv)
        for i in (0, 1):
            pl.when(has_left)(to_right[i].wait_recv)
            pl.when(has_right)(to_left[i].wait_recv)
        image = acc_o[...] + back_r[...] + back_c[...]
        direction = field[...] + ratio[None] * d_ref[...]
        along = image + ratio[None] * along_ref[...]
        d_ref[...] = direction
        along_ref[...] = along
        x_ref[...] += alpha[None] * direction
        left_over = field[...] - alpha[None] * along
        field[...] = left_over
        scal_ref[2, 0:1, :] = lanes(jnp.sum(left_over * left_over, axis=(0, 1))[None])
        cor_near.wait_send()
        pl.when(has_far)(cor_far.wait_send)
        own_near.wait_send()
        pl.when(has_far)(own_far.wait_send)
        for i in (0, 1):
            pl.when(has_right)(to_right[i].wait_send)
            pl.when(has_left)(to_left[i].wait_send)
        shared(msg1, k, n_row, as_, 0)
        shared(msg2, k, n_col, as_, 1)
        return carry

    lax.fori_loop(0, ITERS, iteration, 0)
    x_out[...] = x_ref[...]
    r_out[...] = field[...]


def local(n_row, n_col, right_side, probe, detector_weights, offsets, counts):
    side, cap = probe.shape[1], offsets.shape[2]
    half = side // 2
    field = pltpu.VMEM((2, side, side), f32)
    vmem = pl.BlockSpec(memory_space=pltpu.VMEM)
    smem = pl.BlockSpec(memory_space=pltpu.SMEM)
    shape = jax.ShapeDtypeStruct(right_side.shape, f32)
    return pl.pallas_call(
        functools.partial(kernel, n_row, n_col, cap),
        out_shape=(shape, shape),
        in_specs=[vmem] * 4 + [smem] * 2,
        out_specs=(vmem, vmem),
        scratch_shapes=[field] * 11 + [
            pltpu.VMEM((cap, 2, side, side), f32),
            pltpu.VMEM((cap, 2, side, side), bf16),
            pltpu.VMEM((cap, 2, side, side), bf16),
            pltpu.VMEM((2, side, side), bf16),
            pltpu.VMEM((2, side, side), bf16),
            pltpu.VMEM((side, side), f32),
            field, field, field,
            pltpu.VMEM((1, half), f32),
            pltpu.VMEM((3, 2, half), f32),
            pltpu.VMEM((ITERS, n_row, 2, half), f32),
            pltpu.VMEM((ITERS, n_col, 2, half), f32),
            pltpu.SemaphoreType.DMA((8,)), pltpu.SemaphoreType.DMA((8,)),
            pltpu.SemaphoreType.DMA((8,)), pltpu.SemaphoreType.DMA((8,)),
            pltpu.SemaphoreType.DMA((2, ITERS)), pltpu.SemaphoreType.DMA((2, ITERS)),
        ],
        compiler_params=pltpu.CompilerParams(collective_id=0, has_side_effects=True),
    )(right_side, probe, detector_weights, jnp.asarray(tables(side)), offsets[0, 0], counts)


def solution(mesh):
    in_specs = (P(None, "row", "col"), P(), P(), P("row", "col", None, None), P("row", "col"))
    out_specs = (P(None, "row", "col"), P(None, "row", "col"))
    body = functools.partial(local, mesh.shape["row"], mesh.shape["col"])
    return jax.shard_map(body, mesh=mesh, in_specs=in_specs, out_specs=out_specs, check_vma=False)
```

```python
import functools
import math

import jax
import jax.numpy as jnp
import numpy as np
from jax import lax
from jax.experimental import pallas as pl
from jax.experimental.pallas import tpu as pltpu
from jax.sharding import PartitionSpec as P

ITERS = 3
ridge_weight = 0.5
MESH = pl.DeviceIdType.MESH
f32 = jnp.float32
bf16 = jnp.bfloat16


def tables(side):
    half = side // 2
    n = np.arange(half)
    found = []
    for odd in (0, 1):
        phase = ((2 * np.arange(half) + odd)[:, None] * n[None, :]) % side
        angle = phase * (-2.0 * math.pi / side)
        re, im = np.cos(angle) / math.sqrt(side), np.sin(angle) / math.sqrt(side)
        found.append(np.block([[re, -im], [im, re]]).astype(np.float32))
    full = found + [mat.T.copy() for mat in found]
    out = []
    for mat in full:
        hi = mat.astype(jnp.bfloat16)
        out += [hi, (mat - hi.astype(np.float32)).astype(jnp.bfloat16)]
    return np.stack(out)


def split(value):
    hi = value.astype(bf16)
    return hi, (value - hi.astype(f32)).astype(bf16)


def dot(left, right):
    return jnp.dot(left, right, preferred_element_type=f32)


def kernel(n_row, n_col, cap, right_hbm, probe_hbm, weights_hbm, mats_hbm, offs_ref, count_ref,
           x_out, r_out,
           probe_ref, weights_ref, mats_ref, loads, field, halo_r, halo_c, halo_x, acc_o, acc_r, acc_c, acc_x, back_r, back_c, back_x,
           illum, spec_hi, spec_lo, wave_hi, wave_lo, wgt, x_ref, d_ref, along_ref,
           scal_ref, msg1, msg2, gs, gr, bs, br, as_, ar):
    side = field.shape[1]
    half = side // 2
    row, col = lax.axis_index("row"), lax.axis_index("col")
    odd = lax.rem(row, 2)
    near = row + 1 - 2 * odd
    far = row - 1 + 2 * odd
    has_far = jnp.logical_and(far >= 0, far < n_row)
    has_left, has_right = col > 0, col < n_col - 1
    h_far = pl.multiple_of(odd * half, half)
    h_near = pl.multiple_of(half - odd * half, half)

    fetch = [pltpu.make_async_copy(src, dst, loads.at[i]) for i, (src, dst) in enumerate((
        (right_hbm, field), (probe_hbm, probe_ref), (weights_hbm, weights_ref), (mats_hbm, mats_ref)))]
    for copy in fetch:
        copy.start()
    for ref in (halo_r, halo_c, halo_x, back_r, back_c, back_x):
        ref[...] = jnp.zeros_like(ref)

    barrier = pltpu.get_barrier_semaphore()

    def greet_row(step, carry):
        pl.semaphore_signal(barrier, inc=1, device_id={"row": lax.rem(row + step, n_row)}, device_id_type=MESH)
        return carry

    def greet_col(step, carry):
        pl.semaphore_signal(barrier, inc=1, device_id={"col": lax.rem(col + step, n_col)}, device_id_type=MESH)
        return carry

    lax.fori_loop(1, n_row, greet_row, 0)
    lax.fori_loop(1, n_col, greet_col, 0)
    for ref in (x_ref, d_ref, along_ref):
        ref[...] = jnp.zeros_like(ref)
    fetch[0].wait()
    pl.semaphore_wait(barrier, n_row + n_col - 2)

    def remote(src, dst, sems, rsems, i, target):
        return pltpu.make_async_remote_copy(
            src_ref=src, dst_ref=dst, send_sem=sems.at[i], recv_sem=rsems.at[i],
            device_id=target, device_id_type=MESH)

    quarter = half // 2

    def spans(first, second):
        return [pl.multiple_of(start + i * quarter, quarter) for start in (first, second) for i in (0, 1)]

    def rows_of(ref, start, count=half):
        return ref.at[:, pl.ds(start, count), :]

    def block_of(ref, start, col_start):
        return ref.at[:, pl.ds(start, quarter), pl.ds(col_start, half)]

    def gather_copies():
        left, right = {"col": col - 1}, {"col": col + 1}
        pieces = spans(h_far, h_near)
        to_left = [remote(block_of(field, h, 0), block_of(halo_c, h, 0), gs, gr, i, left)
                   for i, h in enumerate(pieces)]
        to_right = [remote(block_of(field, h, half), block_of(halo_c, h, half), gs, gr, 4 + i, right)
                    for i, h in enumerate(pieces)]
        own_far = remote(rows_of(field, h_far), rows_of(halo_r, h_far), gs, gr, 8, {"row": far})
        own_near = remote(rows_of(field, h_near), rows_of(halo_r, h_near), gs, gr, 9, {"row": near})
        corner = [remote(rows_of(halo_c, h, quarter), rows_of(halo_x, h, quarter), gs, gr, 10 + i,
                         {"row": far if i < 2 else near}) for i, h in enumerate(pieces)]
        return to_left, to_right, own_far, own_near, corner

    def if_far(i, action):
        if i < 2:
            pl.when(has_far)(action)
        else:
            action()

    def gather(between):
        to_left, to_right, own_far, own_near, corner = gather_copies()
        for i in range(4):
            pl.when(has_left)(to_left[i].start)
            pl.when(has_right)(to_right[i].start)
            if i == 0:
                pl.when(has_far)(own_far.start)
                own_near.start()
        between()
        for i in range(4):
            pl.when(has_right)(to_left[i].wait_recv)
            pl.when(has_left)(to_right[i].wait_recv)
            if_far(i, corner[i].start)
        pl.when(has_far)(own_far.wait_recv)
        own_near.wait_recv()
        for i in range(4):
            if_far(i, corner[i].wait_recv)

    def gather_done():
        to_left, to_right, own_far, own_near, corner = gather_copies()
        for i in range(4):
            pl.when(has_left)(to_left[i].wait_send)
            pl.when(has_right)(to_right[i].wait_send)
            if_far(i, corner[i].wait_send)
        pl.when(has_far)(own_far.wait_send)
        own_near.wait_send()

    def prepare():
        for copy in fetch[1:]:
            copy.wait()
        ramp_i = lax.broadcasted_iota(jnp.int32, (side, side), 0)
        ramp_j = lax.broadcasted_iota(jnp.int32, (side, side), 1)
        take = jnp.where(ramp_i < half, 2 * ramp_i, 2 * ramp_i + 1 - side)
        left = jnp.where(take == ramp_j, 1.0, 0.0).astype(f32)
        take_t = jnp.where(ramp_j < half, 2 * ramp_j, 2 * ramp_j + 1 - side)
        right = jnp.where(take_t == ramp_i, 1.0, 0.0).astype(f32)
        moved = jnp.dot(left, weights_ref[...], precision=lax.Precision.HIGHEST, preferred_element_type=f32)
        wgt[...] = jnp.dot(moved, right, precision=lax.Precision.HIGHEST, preferred_element_type=f32)

        def place(s, carry):
            down, across = offs_ref[0, s], offs_ref[1, s]
            down = jnp.where(down < 0, down + side, down)
            across = jnp.where(across < 0, across + side, across)
            flag = jnp.where(s < count_ref[0, 0], 1.0, 0.0).astype(f32)
            for part in (0, 1):
                rolled = pltpu.roll(probe_ref[part] * flag, down, 0)
                illum[s, part] = pltpu.roll(rolled, across, 1)
            return carry

        lax.fori_loop(0, cap, place, 0)
        scal_ref[0] = jnp.ones_like(scal_ref[0])
        scal_ref[1] = jnp.ones_like(scal_ref[1])
        first = field[...]
        scal_ref[2, 0:1, :] = lanes(jnp.sum(first * first, axis=(0, 1))[None])

    def lanes(value):
        return value[:, :half] + value[:, half:]

    def crosses(s, h):
        return s not in (0, 1) or s != h

    def row_mask(s, h):
        t = lax.broadcasted_iota(jnp.int32, (half, half), 0)
        return t >= offs_ref[0, s] if h == 0 else t < offs_ref[0, s] + half

    def col_mask(s, j):
        u = lax.broadcasted_iota(jnp.int32, (half, half), 1)
        return u >= offs_ref[1, s] if j == 0 else u < offs_ref[1, s] + half

    def span(h):
        return slice(h * half, (h + 1) * half)

    def stage_in(s, place):
        for h in (0, 1):
            wave = []
            for j in (0, 1):
                at = (span(h), span(j))
                view = []
                for part in (0, 1):
                    inner = field[part, *at]
                    if crosses(s, h):
                        inner = jnp.where(row_mask(s, h), inner, halo_r[part, *at])
                    if crosses(s, j):
                        outer = halo_c[part, *at]
                        if crosses(s, h):
                            outer = jnp.where(row_mask(s, h), outer, halo_x[part, *at])
                        inner = jnp.where(col_mask(s, j), inner, outer)
                    view.append(inner)
                pr, pi = illum[s, 0, *at], illum[s, 1, *at]
                wave.append((pr * view[0] - pi * view[1], pr * view[1] + pi * view[0]))
            rows = pl.ds(place * side + h * half, half)
            for which, sign in ((0, 1.0), (1, -1.0)):
                for part in (0, 1):
                    hi, lo = split(wave[0][part] + sign * wave[1][part])
                    wave_hi[which, rows, span(part)] = hi
                    wave_lo[which, rows, span(part)] = lo

    def across(mats, which, rows):
        return (dot(wave_hi[which, rows], mats_ref[mats]) + dot(wave_lo[which, rows], mats_ref[mats])
                + dot(wave_hi[which, rows], mats_ref[mats + 1]))

    def down(mats, hi, lo):
        return dot(mats_ref[mats], hi) + dot(mats_ref[mats + 1], hi) + dot(mats_ref[mats], lo)

    def forward(pair, base):
        for i, s in enumerate(pair):
            stage_in(s, base + i)
        rows = pl.ds(base * side, len(pair) * side)
        found = [across(4 + 2 * which, which, rows) for which in (0, 1)]
        quad = jnp.zeros((1, side), f32)
        for i, s in enumerate(pair):
            top, low = i * side, i * side + half
            for which, sign in ((0, 1.0), (1, -1.0)):
                both = [found[j][top:top + half] + sign * found[j][low:low + half] for j in (0, 1)]
                stacked = jnp.concatenate([
                    jnp.concatenate([both[0][:, :half], both[1][:, :half]], axis=1),
                    jnp.concatenate([both[0][:, half:], both[1][:, half:]], axis=1)], axis=0)
                freq = down(2 * which, *split(stacked))
                scale = wgt[span(which), :]
                scaled = freq * jnp.concatenate([scale, scale], axis=0)
                quad = quad + jnp.sum(freq * scaled, axis=0, keepdims=True)
                hi, lo = split(scaled)
                spec_hi[s, which] = hi
                spec_lo[s, which] = lo
        return quad

    def inverse(pair, base):
        for i, s in enumerate(pair):
            even = down(4, spec_hi[s, 0], spec_lo[s, 0])
            odd_ = down(6, spec_hi[s, 1], spec_lo[s, 1])
            for h, sign in ((0, 1.0), (1, -1.0)):
                both = even + sign * odd_
                rows = pl.ds((base + i) * side + h * half, half)
                for j in (0, 1):
                    for part in (0, 1):
                        hi, lo = split(both[span(part), span(j)])
                        wave_hi[j, rows, span(part)] = hi
                        wave_lo[j, rows, span(part)] = lo
        rows = pl.ds(base * side, len(pair) * side)
        out = [across(2 * j, j, rows) for j in (0, 1)]
        for i, s in enumerate(pair):
            for h in (0, 1):
                mine = slice(i * side + h * half, i * side + (h + 1) * half)
                for j, sign in ((0, 1.0), (1, -1.0)):
                    at = (span(h), span(j))
                    mixed = out[0][mine] + sign * out[1][mine]
                    hr, hi = mixed[:, :half], mixed[:, half:]
                    pr, pi = illum[s, 0, *at], illum[s, 1, *at]
                    for part, term in ((0, pr * hr + pi * hi), (1, pr * hi - pi * hr)):
                        scatter(s, h, j, part, term)

    def add_to(ref, s, first, part, at, value):
        if s == first:
            ref[part, *at] = value
        else:
            ref[part, *at] += value

    def scatter(s, h, j, part, term):
        at = (span(h), span(j))
        inner = term
        if crosses(s, h):
            inner = jnp.where(row_mask(s, h), term, 0.0)
            outer = term - inner
            if crosses(s, j):
                kept = jnp.where(col_mask(s, j), outer, 0.0)
                add_to(acc_x, s, min(t for t in range(cap) if crosses(t, h) and crosses(t, j)), part, at, outer - kept)
                outer = kept
            add_to(acc_r, s, min(t for t in range(cap) if crosses(t, h)), part, at, outer)
        if crosses(s, j):
            kept = jnp.where(col_mask(s, j), inner, 0.0)
            add_to(acc_c, s, min(t for t in range(cap) if crosses(t, j)), part, at, inner - kept)
            inner = kept
        if s == 0:
            inner = inner + ridge_weight * field[part, *at]
        add_to(acc_o, s, 0, part, at, inner)

    def share(msg, mine, k, count, axis, at, i):
        def send(step, carry):
            remote_to = {axis: lax.rem(mine + step, count)}
            pltpu.make_async_remote_copy(
                src_ref=msg.at[k, mine], dst_ref=msg.at[k, mine], send_sem=as_.at[i, k], recv_sem=ar.at[i, k],
                device_id=remote_to, device_id_type=MESH).start()
            return carry
        msg[k, at] = scal_ref[2]
        lax.fori_loop(1, count, send, 0)

    def shared(msg, k, count, sem, i):
        part = msg.at[k, pl.ds(0, count - 1)]
        pltpu.make_async_copy(part, part, sem.at[i, k]).wait()

    def back_copies():
        left, right = {"col": col - 1}, {"col": col + 1}
        out = spans(h_near, h_far)
        corner = [remote(rows_of(acc_x, h, quarter), rows_of(back_x, h, quarter), bs, br, i,
                         {"row": far if i < 2 else near}) for i, h in enumerate(out)]
        own_far = remote(rows_of(acc_r, h_near), rows_of(back_r, h_near), bs, br, 4, {"row": far})
        own_near = remote(rows_of(acc_r, h_far), rows_of(back_r, h_far), bs, br, 5, {"row": near})
        to_right = [remote(block_of(acc_c, h, 0), block_of(back_c, h, 0), bs, br, 6 + i, right)
                    for i, h in enumerate(out)]
        to_left = [remote(block_of(acc_c, h, half), block_of(back_c, h, half), bs, br, 10 + i, left)
                   for i, h in enumerate(out)]
        return corner, own_far, own_near, to_right, to_left, out

    def iteration(k, carry):
        gather(lambda: pl.when(k == 0)(prepare))
        pairs = [tuple(range(s, min(s + 2, cap))) for s in range(0, cap, 2)]
        quad = sum(forward(pair, pair[0]) for pair in pairs)
        scal_ref[2, 1:2, :] = lanes(quad) + ridge_weight * scal_ref[2, 0:1, :]
        share(msg1, col, k, n_col, "col", col, 0)
        gather_done()
        for pair in pairs:
            inverse(pair, pair[0])

        corner, own_far, own_near, to_right, to_left, out = back_copies()
        for i in range(4):
            if_far(i, corner[i].start)
        pl.when(has_far)(own_far.start)
        own_near.start()
        for i, h in enumerate(out):
            if_far((i + 2) % 4, corner[(i + 2) % 4].wait_recv)
            acc_c[:, pl.ds(h, quarter), :] += back_x[:, pl.ds(h, quarter), :]
            pl.when(has_right)(to_right[i].start)
            pl.when(has_left)(to_left[i].start)
            if i == 1:
                shared(msg1, k, n_col, ar, 0)
                scal_ref[2] = jnp.sum(msg1[k], axis=0)
                share(msg2, row, k, n_row, "row", row, 1)
        shared(msg2, k, n_row, ar, 1)
        total = jnp.sum(jnp.sum(msg2[k], axis=0), axis=1, keepdims=True)
        norm, product = total[0:1], total[1:2]
        before, alpha_before = scal_ref[0, 0:1, 0:1], scal_ref[1, 0:1, 0:1]
        ratio = jnp.where(k == 0, jnp.zeros_like(norm), norm / before)
        alpha = norm / (product - ratio * norm / alpha_before)
        scal_ref[0] = jnp.broadcast_to(norm, scal_ref.shape[1:])
        scal_ref[1] = jnp.broadcast_to(alpha, scal_ref.shape[1:])
        own_near.wait_recv()
        pl.when(has_far)(own_far.wait_recv)
        for i in range(4):
            pl.when(has_left)(to_right[i].wait_recv)
            pl.when(has_right)(to_left[i].wait_recv)
        image = acc_o[...] + back_r[...] + back_c[...]
        direction = field[...] + ratio[None] * d_ref[...]
        along = image + ratio[None] * along_ref[...]
        d_ref[...] = direction
        along_ref[...] = along
        x_ref[...] += alpha[None] * direction
        left_over = field[...] - alpha[None] * along
        field[...] = left_over
        scal_ref[2, 0:1, :] = lanes(jnp.sum(left_over * left_over, axis=(0, 1))[None])
        for i in range(4):
            if_far(i, corner[i].wait_send)
            pl.when(has_right)(to_right[i].wait_send)
            pl.when(has_left)(to_left[i].wait_send)
        own_near.wait_send()
        pl.when(has_far)(own_far.wait_send)
        shared(msg1, k, n_col, as_, 0)
        shared(msg2, k, n_row, as_, 1)
        return carry

    lax.fori_loop(0, ITERS, iteration, 0)
    x_out[...] = x_ref[...]
    r_out[...] = field[...]


def local(n_row, n_col, right_side, probe, detector_weights, offsets, counts):
    side, cap = probe.shape[1], offsets.shape[2]
    half = side // 2
    field = pltpu.VMEM((2, side, side), f32)
    vmem = pl.BlockSpec(memory_space=pltpu.VMEM)
    smem = pl.BlockSpec(memory_space=pltpu.SMEM)
    shape = pltpu.VMEM(right_side.shape, f32)
    return pl.pallas_call(
        functools.partial(kernel, n_row, n_col, cap),
        out_shape=(shape, shape),
        in_specs=[pl.BlockSpec(memory_space=pltpu.HBM)] * 4 + [smem] * 2,
        out_specs=(vmem, vmem),
        scratch_shapes=[
            field, pltpu.VMEM((side, side), f32), pltpu.VMEM((8, side, side), bf16), pltpu.SemaphoreType.DMA((4,)),
        ] + [field] * 11 + [
            pltpu.VMEM((cap, 2, side, side), f32),
            pltpu.VMEM((cap, 2, side, side), bf16),
            pltpu.VMEM((cap, 2, side, side), bf16),
            pltpu.VMEM((2, cap * side, side), bf16),
            pltpu.VMEM((2, cap * side, side), bf16),
            pltpu.VMEM((side, side), f32),
            field, field, field,
            pltpu.VMEM((3, 2, half), f32),
            pltpu.VMEM((ITERS, n_col, 2, half), f32),
            pltpu.VMEM((ITERS, n_row, 2, half), f32),
            pltpu.SemaphoreType.DMA((14,)), pltpu.SemaphoreType.DMA((14,)),
            pltpu.SemaphoreType.DMA((14,)), pltpu.SemaphoreType.DMA((14,)),
            pltpu.SemaphoreType.DMA((2, ITERS)), pltpu.SemaphoreType.DMA((2, ITERS)),
        ],
        compiler_params=pltpu.CompilerParams(collective_id=0, has_side_effects=True),
    )(right_side, probe, detector_weights, jnp.asarray(tables(side)), offsets[0, 0].T, counts)


def solution(mesh):
    in_specs = (P(None, "row", "col"), P(), P(), P("row", "col", None, None), P("row", "col"))
    out_specs = (P(None, "row", "col"), P(None, "row", "col"))
    body = functools.partial(local, mesh.shape["row"], mesh.shape["col"])
    return jax.shard_map(body, mesh=mesh, in_specs=in_specs, out_specs=out_specs, check_vma=False)
```

```python
import functools
import math

import jax
import jax.numpy as jnp
import numpy as np
from jax import lax
from jax.experimental import pallas as pl
from jax.experimental.pallas import tpu as pltpu
from jax.sharding import PartitionSpec as P

ITERS = 3
ridge_weight = 0.5
MESH = pl.DeviceIdType.MESH
f32 = jnp.float32
bf16 = jnp.bfloat16


def tables(side):
    half = side // 2
    n = np.arange(half)
    found = []
    for odd in (0, 1):
        phase = ((2 * np.arange(half) + odd)[:, None] * n[None, :]) % side
        angle = phase * (-2.0 * math.pi / side)
        re, im = np.cos(angle) / math.sqrt(side), np.sin(angle) / math.sqrt(side)
        found.append(np.block([[re, -im], [im, re]]).astype(np.float32))
    full = found + [mat.T.copy() for mat in found]
    out = []
    for mat in full:
        hi = mat.astype(jnp.bfloat16)
        out += [hi, (mat - hi.astype(np.float32)).astype(jnp.bfloat16)]
    return np.stack(out)


def split(value):
    hi = value.astype(bf16)
    return hi, (value - hi.astype(f32)).astype(bf16)


def dot(left, right):
    return jnp.dot(left, right, preferred_element_type=f32)


def kernel(n_row, n_col, cap, right_hbm, probe_hbm, weights_hbm, mats_hbm, offs_hbm, count_hbm,
           x_out, r_out,
           probe_ref, weights_ref, mats_ref, offs_ref, count_ref, loads, field, halo_r, halo_c, halo_x, acc_o, acc_r, acc_c, acc_x, back_r, back_c, back_x,
           illum, spec_hi, spec_lo, wave_hi, wave_lo, wgt, x_ref, d_ref, along_ref,
           scal_ref, msg1, msg2, gs, gr, bs, br, as_, ar):
    side = field.shape[1]
    half = side // 2
    row, col = lax.axis_index("row"), lax.axis_index("col")
    odd = lax.rem(row, 2)
    near = row + 1 - 2 * odd
    far = row - 1 + 2 * odd
    has_far = jnp.logical_and(far >= 0, far < n_row)
    has_left, has_right = col > 0, col < n_col - 1
    h_far = pl.multiple_of(odd * half, half)
    h_near = pl.multiple_of(half - odd * half, half)

    fetch = [pltpu.make_async_copy(src, dst, loads.at[i]) for i, (src, dst) in enumerate((
        (right_hbm, field), (probe_hbm, probe_ref), (weights_hbm, weights_ref),
        (mats_hbm, mats_ref), (offs_hbm, offs_ref), (count_hbm, count_ref)))]
    for copy in fetch:
        copy.start()
    for ref in (halo_r, halo_c, halo_x, back_r, back_c, back_x):
        ref[...] = jnp.zeros_like(ref)

    barrier = pltpu.get_barrier_semaphore()

    def greet_row(step, carry):
        pl.semaphore_signal(barrier, inc=1, device_id={"row": lax.rem(row + step, n_row)}, device_id_type=MESH)
        return carry

    def greet_col(step, carry):
        pl.semaphore_signal(barrier, inc=1, device_id={"col": lax.rem(col + step, n_col)}, device_id_type=MESH)
        return carry

    lax.fori_loop(1, n_row, greet_row, 0)
    lax.fori_loop(1, n_col, greet_col, 0)
    for ref in (x_ref, d_ref, along_ref):
        ref[...] = jnp.zeros_like(ref)
    fetch[0].wait()
    pl.semaphore_wait(barrier, n_row + n_col - 2)

    def remote(src, dst, sems, rsems, i, target):
        return pltpu.make_async_remote_copy(
            src_ref=src, dst_ref=dst, send_sem=sems.at[i], recv_sem=rsems.at[i],
            device_id=target, device_id_type=MESH)

    fine = half // 4
    even_cut = [(i * fine, fine) for i in range(4)]
    late_cut = [(0, 2 * fine), (2 * fine, fine), (3 * fine, fine)]
    early_cut = [(0, fine), (fine, fine), (2 * fine, 2 * fine)]

    def spans(*groups):
        return [(pl.multiple_of(start + at, fine), size) for start, cut in groups for at, size in cut]

    def rows_of(ref, start, count=half):
        return ref.at[:, pl.ds(start, count), :]

    def block_of(ref, piece, col_start):
        return ref.at[:, pl.ds(*piece), pl.ds(col_start, half)]

    n_far = len(even_cut)
    n_near = len(late_cut)
    n_all = n_far + n_near
    gather_pieces = spans((h_far, even_cut), (h_near, late_cut))
    back_pieces = spans((h_near, early_cut), (h_far, even_cut))

    left, right = {"col": col - 1}, {"col": col + 1}
    to_left = [remote(block_of(field, h, 0), block_of(halo_c, h, 0), gs, gr, i, left)
               for i, h in enumerate(gather_pieces)]
    to_right = [remote(block_of(field, h, half), block_of(halo_c, h, half), gs, gr, n_all + i, right)
                for i, h in enumerate(gather_pieces)]
    own_far = remote(rows_of(field, h_far), rows_of(halo_r, h_far), gs, gr, 2 * n_all, {"row": far})
    own_near = remote(rows_of(field, h_near), rows_of(halo_r, h_near), gs, gr, 2 * n_all + 1, {"row": near})
    corner = [remote(rows_of(halo_c, *h), rows_of(halo_x, *h), gs, gr, 2 * n_all + 2 + i,
                     {"row": far if i < n_far else near}) for i, h in enumerate(gather_pieces)]

    def if_far(i, action):
        if i < n_far:
            pl.when(has_far)(action)
        else:
            action()

    def send_piece(i, going):
        pl.when(jnp.logical_and(going, has_left))(to_left[i].start)
        pl.when(jnp.logical_and(going, has_right))(to_right[i].start)
        if i == n_far - 1:
            pl.when(jnp.logical_and(going, has_far))(own_far.start)
        if i == n_all - 1:
            pl.when(going)(own_near.start)

    def gather():
        for i in range(n_all):
            pl.when(has_right)(to_left[i].wait_recv)
            pl.when(has_left)(to_right[i].wait_recv)
            if_far(i, corner[i].start)
        pl.when(has_far)(own_far.wait_recv)
        own_near.wait_recv()
        for i in range(n_all):
            if_far(i, corner[i].wait_recv)

    def gather_done():
        for i in range(n_all):
            pl.when(has_left)(to_left[i].wait_send)
            pl.when(has_right)(to_right[i].wait_send)
            if_far(i, corner[i].wait_send)
        pl.when(has_far)(own_far.wait_send)
        own_near.wait_send()

    far_out = spans((h_near, even_cut))
    near_out = spans((h_far, early_cut))
    back_far = [remote(rows_of(acc_x, *h), rows_of(back_x, *h), bs, br, i, {"row": far})
                for i, h in enumerate(far_out)]
    back_near = [remote(rows_of(acc_x, *h), rows_of(back_x, *h), bs, br, n_far + i, {"row": near})
                 for i, h in enumerate(near_out)]
    row_far = remote(rows_of(acc_r, h_near), rows_of(back_r, h_near), bs, br, n_all, {"row": far})
    row_near = remote(rows_of(acc_r, h_far), rows_of(back_r, h_far), bs, br, n_all + 1, {"row": near})
    col_right = [remote(block_of(acc_c, h, 0), block_of(back_c, h, 0), bs, br, n_all + 2 + i, right)
                 for i, h in enumerate(back_pieces)]
    col_left = [remote(block_of(acc_c, h, half), block_of(back_c, h, half), bs, br, 2 * n_all + 2 + i, left)
                for i, h in enumerate(back_pieces)]

    def prepare():
        for copy in fetch[1:]:
            copy.wait()
        ramp_i = lax.broadcasted_iota(jnp.int32, (side, side), 0)
        ramp_j = lax.broadcasted_iota(jnp.int32, (side, side), 1)
        take = jnp.where(ramp_i < half, 2 * ramp_i, 2 * ramp_i + 1 - side)
        left = jnp.where(take == ramp_j, 1.0, 0.0).astype(f32)
        take_t = jnp.where(ramp_j < half, 2 * ramp_j, 2 * ramp_j + 1 - side)
        right = jnp.where(take_t == ramp_i, 1.0, 0.0).astype(f32)
        moved = jnp.dot(left, weights_ref[...], precision=lax.Precision.HIGHEST, preferred_element_type=f32)
        wgt[...] = jnp.dot(moved, right, precision=lax.Precision.HIGHEST, preferred_element_type=f32)

        def place(s, carry):
            down, across = offs_ref[0, s], offs_ref[1, s]
            down = jnp.where(down < 0, down + side, down)
            across = jnp.where(across < 0, across + side, across)
            flag = jnp.where(s < count_ref[0, 0], 1.0, 0.0).astype(f32)
            for part in (0, 1):
                rolled = pltpu.roll(probe_ref[part] * flag, down, 0)
                illum[s, part] = pltpu.roll(rolled, across, 1)
            return carry

        lax.fori_loop(0, cap, place, 0)
        scal_ref[0] = jnp.ones_like(scal_ref[0])
        scal_ref[1] = jnp.ones_like(scal_ref[1])
        first = field[...]
        scal_ref[2, 0:1, :] = lanes(jnp.sum(first * first, axis=(0, 1))[None])

    def lanes(value):
        return value[:, :half] + value[:, half:]

    def crosses(s, h):
        return s not in (0, 1) or s != h

    def row_mask(s, h):
        t = lax.broadcasted_iota(jnp.int32, (half, half), 0)
        return t >= offs_ref[0, s] if h == 0 else t < offs_ref[0, s] + half

    def col_mask(s, j):
        u = lax.broadcasted_iota(jnp.int32, (half, half), 1)
        return u >= offs_ref[1, s] if j == 0 else u < offs_ref[1, s] + half

    def span(h):
        return slice(h * half, (h + 1) * half)

    def stage_in(s, place):
        for h in (0, 1):
            wave = []
            for j in (0, 1):
                at = (span(h), span(j))
                view = []
                for part in (0, 1):
                    inner = field[part, *at]
                    if crosses(s, h):
                        inner = jnp.where(row_mask(s, h), inner, halo_r[part, *at])
                    if crosses(s, j):
                        outer = halo_c[part, *at]
                        if crosses(s, h):
                            outer = jnp.where(row_mask(s, h), outer, halo_x[part, *at])
                        inner = jnp.where(col_mask(s, j), inner, outer)
                    view.append(inner)
                pr, pi = illum[s, 0, *at], illum[s, 1, *at]
                wave.append((pr * view[0] - pi * view[1], pr * view[1] + pi * view[0]))
            rows = pl.ds(place * side + h * half, half)
            for which, sign in ((0, 1.0), (1, -1.0)):
                for part in (0, 1):
                    hi, lo = split(wave[0][part] + sign * wave[1][part])
                    wave_hi[which, rows, span(part)] = hi
                    wave_lo[which, rows, span(part)] = lo

    def across(mats, which, rows):
        return (dot(wave_hi[which, rows], mats_ref[mats]) + dot(wave_lo[which, rows], mats_ref[mats])
                + dot(wave_hi[which, rows], mats_ref[mats + 1]))

    def down(mats, hi, lo):
        return dot(mats_ref[mats], hi) + dot(mats_ref[mats + 1], hi) + dot(mats_ref[mats], lo)

    def forward(pair, base):
        for i, s in enumerate(pair):
            stage_in(s, base + i)
        rows = pl.ds(base * side, len(pair) * side)
        found = [across(4 + 2 * which, which, rows) for which in (0, 1)]
        quad = jnp.zeros((1, side), f32)
        for i, s in enumerate(pair):
            top, low = i * side, i * side + half
            for which, sign in ((0, 1.0), (1, -1.0)):
                both = [found[j][top:top + half] + sign * found[j][low:low + half] for j in (0, 1)]
                stacked = jnp.concatenate([
                    jnp.concatenate([both[0][:, :half], both[1][:, :half]], axis=1),
                    jnp.concatenate([both[0][:, half:], both[1][:, half:]], axis=1)], axis=0)
                freq = down(2 * which, *split(stacked))
                scale = wgt[span(which), :]
                scaled = freq * jnp.concatenate([scale, scale], axis=0)
                quad = quad + jnp.sum(freq * scaled, axis=0, keepdims=True)
                hi, lo = split(scaled)
                spec_hi[s, which] = hi
                spec_lo[s, which] = lo
        return quad

    def inverse(pair, base):
        for i, s in enumerate(pair):
            even = down(4, spec_hi[s, 0], spec_lo[s, 0])
            odd_ = down(6, spec_hi[s, 1], spec_lo[s, 1])
            for h, sign in ((0, 1.0), (1, -1.0)):
                both = even + sign * odd_
                rows = pl.ds((base + i) * side + h * half, half)
                for j in (0, 1):
                    for part in (0, 1):
                        hi, lo = split(both[span(part), span(j)])
                        wave_hi[j, rows, span(part)] = hi
                        wave_lo[j, rows, span(part)] = lo
        rows = pl.ds(base * side, len(pair) * side)
        out = [across(2 * j, j, rows) for j in (0, 1)]
        for i, s in enumerate(pair):
            for h in (0, 1):
                mine = slice(i * side + h * half, i * side + (h + 1) * half)
                for j, sign in ((0, 1.0), (1, -1.0)):
                    at = (span(h), span(j))
                    mixed = out[0][mine] + sign * out[1][mine]
                    hr, hi = mixed[:, :half], mixed[:, half:]
                    pr, pi = illum[s, 0, *at], illum[s, 1, *at]
                    for part, term in ((0, pr * hr + pi * hi), (1, pr * hi - pi * hr)):
                        scatter(s, h, j, part, term)

    def add_to(ref, s, first, part, at, value):
        if s == first:
            ref[part, *at] = value
        else:
            ref[part, *at] += value

    def scatter(s, h, j, part, term):
        at = (span(h), span(j))
        inner = term
        if crosses(s, h):
            inner = jnp.where(row_mask(s, h), term, 0.0)
            outer = term - inner
            if crosses(s, j):
                kept = jnp.where(col_mask(s, j), outer, 0.0)
                add_to(acc_x, s, min(t for t in range(cap) if crosses(t, h) and crosses(t, j)), part, at, outer - kept)
                outer = kept
            add_to(acc_r, s, min(t for t in range(cap) if crosses(t, h)), part, at, outer)
        if crosses(s, j):
            kept = jnp.where(col_mask(s, j), inner, 0.0)
            add_to(acc_c, s, min(t for t in range(cap) if crosses(t, j)), part, at, inner - kept)
            inner = kept
        if s == 0:
            inner = inner + ridge_weight * field[part, *at]
        add_to(acc_o, s, 0, part, at, inner)

    def share(msg, mine, k, count, axis, at, i):
        def send(step, carry):
            remote_to = {axis: lax.rem(mine + step, count)}
            pltpu.make_async_remote_copy(
                src_ref=msg.at[k, mine], dst_ref=msg.at[k, mine], send_sem=as_.at[i, k], recv_sem=ar.at[i, k],
                device_id=remote_to, device_id_type=MESH).start()
            return carry
        msg[k, at] = scal_ref[2]
        lax.fori_loop(1, count, send, 0)

    def shared(msg, k, count, sem, i):
        part = msg.at[k, pl.ds(0, count - 1)]
        pltpu.make_async_copy(part, part, sem.at[i, k]).wait()

    def iteration(k, carry):
        pl.when(k == 0)(prepare)
        gather()
        pairs = [tuple(range(s, min(s + 2, cap))) for s in range(0, cap, 2)]
        quad = sum(forward(pair, pair[0]) for pair in pairs)
        scal_ref[2, 1:2, :] = lanes(quad) + ridge_weight * scal_ref[2, 0:1, :]
        share(msg1, col, k, n_col, "col", col, 0)
        gather_done()
        for pair in pairs:
            inverse(pair, pair[0])

        for copy in back_near:
            copy.start()
        for copy in back_far:
            pl.when(has_far)(copy.start)
        row_near.start()
        for i, (start, size) in enumerate(back_pieces):
            if i < n_near:
                back_near[i].wait_recv()
            else:
                pl.when(has_far)(back_far[i - n_near].wait_recv)
            acc_c[:, pl.ds(start, size), :] += back_x[:, pl.ds(start, size), :]
            pl.when(has_right)(col_right[i].start)
            pl.when(has_left)(col_left[i].start)
            if i == n_near - 1:
                shared(msg1, k, n_col, ar, 0)
                scal_ref[2] = jnp.sum(msg1[k], axis=0)
                share(msg2, row, k, n_row, "row", row, 1)
                pl.when(has_far)(row_far.start)
        shared(msg2, k, n_row, ar, 1)
        total = jnp.sum(jnp.sum(msg2[k], axis=0), axis=1, keepdims=True)
        norm, product = total[0:1], total[1:2]
        norm_before, alpha_before = scal_ref[0, 0:1, 0:1], scal_ref[1, 0:1, 0:1]
        ratio = jnp.where(k == 0, jnp.zeros_like(norm), norm / norm_before)
        alpha = norm / (product - ratio * norm / alpha_before)
        scal_ref[0] = jnp.broadcast_to(norm, scal_ref.shape[1:])
        scal_ref[1] = jnp.broadcast_to(alpha, scal_ref.shape[1:])
        row_near.wait_recv()
        pl.when(has_far)(row_far.wait_recv)
        for i in range(n_all):
            pl.when(has_left)(col_right[i].wait_recv)
            pl.when(has_right)(col_left[i].wait_recv)
        square = jnp.zeros((1, side), f32)
        going = k + 1 < ITERS
        for i, (start, size) in enumerate(gather_pieces):
            rows = pl.ds(start, size)
            before = field[:, rows, :]
            image = acc_o[:, rows, :] + back_r[:, rows, :] + back_c[:, rows, :]
            direction = before + ratio[None] * d_ref[:, rows, :]
            along = image + ratio[None] * along_ref[:, rows, :]
            d_ref[:, rows, :] = direction
            along_ref[:, rows, :] = along
            x_ref[:, rows, :] += alpha[None] * direction
            left_over = before - alpha[None] * along
            field[:, rows, :] = left_over
            square = square + jnp.sum(left_over * left_over, axis=(0, 1))[None]
            if i > 0:
                send_piece(i - 1, going)
        send_piece(n_all - 1, going)
        scal_ref[2, 0:1, :] = lanes(square)
        for copy in back_near:
            copy.wait_send()
        for copy in back_far:
            pl.when(has_far)(copy.wait_send)
        row_near.wait_send()
        pl.when(has_far)(row_far.wait_send)
        for i in range(n_all):
            pl.when(has_right)(col_right[i].wait_send)
            pl.when(has_left)(col_left[i].wait_send)
        shared(msg1, k, n_col, as_, 0)
        shared(msg2, k, n_row, as_, 1)
        return carry

    for i in range(n_all):
        send_piece(i, True)
    lax.fori_loop(0, ITERS, iteration, 0)
    x_out[...] = x_ref[...]
    r_out[...] = field[...]


def local(n_row, n_col, right_side, probe, detector_weights, offsets, counts):
    side, cap = probe.shape[1], offsets.shape[2]
    half = side // 2
    field = pltpu.VMEM((2, side, side), f32)
    vmem = pl.BlockSpec(memory_space=pltpu.VMEM)
    shape = pltpu.VMEM(right_side.shape, f32)
    return pl.pallas_call(
        functools.partial(kernel, n_row, n_col, cap),
        out_shape=(shape, shape),
        in_specs=[pl.BlockSpec(memory_space=pltpu.HBM)] * 6,
        out_specs=(vmem, vmem),
        scratch_shapes=[
            field, pltpu.VMEM((side, side), f32), pltpu.VMEM((8, side, side), bf16),
            pltpu.SMEM((2, cap), jnp.int32), pltpu.SMEM((1, 1), jnp.int32), pltpu.SemaphoreType.DMA((6,)),
        ] + [field] * 11 + [
            pltpu.VMEM((cap, 2, side, side), f32),
            pltpu.VMEM((cap, 2, side, side), bf16),
            pltpu.VMEM((cap, 2, side, side), bf16),
            pltpu.VMEM((2, cap * side, side), bf16),
            pltpu.VMEM((2, cap * side, side), bf16),
            pltpu.VMEM((side, side), f32),
            field, field, field,
            pltpu.VMEM((3, 2, half), f32),
            pltpu.VMEM((ITERS, n_col, 2, half), f32),
            pltpu.VMEM((ITERS, n_row, 2, half), f32),
            pltpu.SemaphoreType.DMA((23,)), pltpu.SemaphoreType.DMA((23,)),
            pltpu.SemaphoreType.DMA((23,)), pltpu.SemaphoreType.DMA((23,)),
            pltpu.SemaphoreType.DMA((2, ITERS)), pltpu.SemaphoreType.DMA((2, ITERS)),
        ],
        compiler_params=pltpu.CompilerParams(collective_id=0, has_side_effects=True),
    )(right_side, probe, detector_weights, jnp.asarray(tables(side)), offsets[0, 0].T, counts)


def solution(mesh):
    in_specs = (P(None, "row", "col"), P(), P(), P("row", "col", None, None), P("row", "col"))
    out_specs = (P(None, "row", "col"), P(None, "row", "col"))
    body = functools.partial(local, mesh.shape["row"], mesh.shape["col"])
    return jax.shard_map(body, mesh=mesh, in_specs=in_specs, out_specs=out_specs, check_vma=False)
```

```python
import functools
import math

import jax
import jax.numpy as jnp
import numpy as np
from jax import lax
from jax.experimental import pallas as pl
from jax.experimental.pallas import tpu as pltpu
from jax.sharding import PartitionSpec as P

ITERS = 3
ridge_weight = 0.5
MESH = pl.DeviceIdType.MESH
f32 = jnp.float32
bf16 = jnp.bfloat16


def tables(side):
    half = side // 2
    n = np.arange(half)
    found = []
    for odd in (0, 1):
        phase = ((2 * np.arange(half) + odd)[:, None] * n[None, :]) % side
        angle = phase * (-2.0 * math.pi / side)
        re, im = np.cos(angle) / math.sqrt(side), np.sin(angle) / math.sqrt(side)
        found.append(np.block([[re, -im], [im, re]]).astype(np.float32))
    full = found + [mat.T.copy() for mat in found]
    out = []
    for mat in full:
        hi = mat.astype(jnp.bfloat16)
        out += [hi, (mat - hi.astype(np.float32)).astype(jnp.bfloat16)]
    return np.stack([np.stack([mat[:, :half], mat[:, half:]]) for mat in out])


def split(value):
    hi = value.astype(bf16)
    return hi, (value - hi.astype(f32)).astype(bf16)


def dot(left, right):
    return jnp.dot(left, right, preferred_element_type=f32)


def kernel(n_row, n_col, cap, right_hbm, probe_hbm, weights_hbm, mats_hbm, offs_hbm, count_hbm,
           x_out, r_out,
           probe_ref, weights_ref, mats_ref, offs_ref, count_ref, loads, field, halo_r, halo_c, halo_x, acc_o, acc_r, acc_c, acc_x, back_r, back_c, back_x,
           illum, spec_hi, spec_lo, wave_hi, wave_lo, wgt, x_ref, d_ref, along_ref,
           scal_ref, msg1, msg2, gs, gr, bs, br, as_, ar):
    side = field.shape[1]
    half = side // 2
    row, col = lax.axis_index("row"), lax.axis_index("col")
    odd = lax.rem(row, 2)
    near = row + 1 - 2 * odd
    far = row - 1 + 2 * odd
    has_far = jnp.logical_and(far >= 0, far < n_row)
    has_left, has_right = col > 0, col < n_col - 1
    h_far = pl.multiple_of(odd * half, half)
    h_near = pl.multiple_of(half - odd * half, half)

    fetch = [pltpu.make_async_copy(src, dst, loads.at[i]) for i, (src, dst) in enumerate((
        (right_hbm, field), (probe_hbm, probe_ref), (weights_hbm, weights_ref),
        (mats_hbm, mats_ref), (offs_hbm, offs_ref), (count_hbm, count_ref)))]
    for copy in fetch:
        copy.start()
    for ref in (halo_r, halo_c, halo_x, back_r, back_c, back_x):
        ref[...] = jnp.zeros_like(ref)

    barrier = pltpu.get_barrier_semaphore()

    def greet_row(step, carry):
        pl.semaphore_signal(barrier, inc=1, device_id={"row": lax.rem(row + step, n_row)}, device_id_type=MESH)
        return carry

    def greet_col(step, carry):
        pl.semaphore_signal(barrier, inc=1, device_id={"col": lax.rem(col + step, n_col)}, device_id_type=MESH)
        return carry

    lax.fori_loop(1, n_row, greet_row, 0)
    lax.fori_loop(1, n_col, greet_col, 0)
    for ref in (x_ref, d_ref, along_ref):
        ref[...] = jnp.zeros_like(ref)
    fetch[0].wait()
    pl.semaphore_wait(barrier, n_row + n_col - 2)

    def remote(src, dst, sems, rsems, i, target):
        return pltpu.make_async_remote_copy(
            src_ref=src, dst_ref=dst, send_sem=sems.at[i], recv_sem=rsems.at[i],
            device_id=target, device_id_type=MESH)

    fine = half // 4
    even_cut = [(i * fine, fine) for i in range(4)]
    late_cut = [(0, 2 * fine), (2 * fine, fine), (3 * fine, fine)]
    early_cut = [(0, fine), (fine, fine), (2 * fine, 2 * fine)]

    def spans(*groups):
        return [(pl.multiple_of(start + at, fine), size) for start, cut in groups for at, size in cut]

    def rows_of(ref, start, count=half):
        return ref.at[:, pl.ds(start, count), :]

    def block_of(ref, piece, col_start):
        return ref.at[:, pl.ds(*piece), pl.ds(col_start, half)]

    n_far = len(even_cut)
    n_near = len(late_cut)
    n_all = n_far + n_near
    gather_pieces = spans((h_far, even_cut), (h_near, late_cut))
    back_pieces = spans((h_near, early_cut), (h_far, even_cut))

    left, right = {"col": col - 1}, {"col": col + 1}
    to_left = [remote(block_of(field, h, 0), block_of(halo_c, h, 0), gs, gr, i, left)
               for i, h in enumerate(gather_pieces)]
    to_right = [remote(block_of(field, h, half), block_of(halo_c, h, half), gs, gr, n_all + i, right)
                for i, h in enumerate(gather_pieces)]
    own_far = remote(rows_of(field, h_far), rows_of(halo_r, h_far), gs, gr, 2 * n_all, {"row": far})
    own_near = remote(rows_of(field, h_near), rows_of(halo_r, h_near), gs, gr, 2 * n_all + 1, {"row": near})
    corner = [remote(rows_of(halo_c, *h), rows_of(halo_x, *h), gs, gr, 2 * n_all + 2 + i,
                     {"row": far if i < n_far else near}) for i, h in enumerate(gather_pieces)]

    def if_far(i, action):
        if i < n_far:
            pl.when(has_far)(action)
        else:
            action()

    def send_piece(i, going):
        pl.when(jnp.logical_and(going, has_left))(to_left[i].start)
        pl.when(jnp.logical_and(going, has_right))(to_right[i].start)
        if i == n_far - 1:
            pl.when(jnp.logical_and(going, has_far))(own_far.start)
        if i == n_all - 1:
            pl.when(going)(own_near.start)

    def gather():
        for i in range(n_all):
            pl.when(has_right)(to_left[i].wait_recv)
            pl.when(has_left)(to_right[i].wait_recv)
            if_far(i, corner[i].start)
        pl.when(has_far)(own_far.wait_recv)
        own_near.wait_recv()
        for i in range(n_all):
            if_far(i, corner[i].wait_recv)

    def gather_done():
        for i in range(n_all):
            pl.when(has_left)(to_left[i].wait_send)
            pl.when(has_right)(to_right[i].wait_send)
            if_far(i, corner[i].wait_send)
        pl.when(has_far)(own_far.wait_send)
        own_near.wait_send()

    far_out = spans((h_near, even_cut))
    near_out = spans((h_far, early_cut))
    back_far = [remote(rows_of(acc_x, *h), rows_of(back_x, *h), bs, br, i, {"row": far})
                for i, h in enumerate(far_out)]
    back_near = [remote(rows_of(acc_x, *h), rows_of(back_x, *h), bs, br, n_far + i, {"row": near})
                 for i, h in enumerate(near_out)]
    row_far = remote(rows_of(acc_r, h_near), rows_of(back_r, h_near), bs, br, n_all, {"row": far})
    row_near = remote(rows_of(acc_r, h_far), rows_of(back_r, h_far), bs, br, n_all + 1, {"row": near})
    col_right = [remote(block_of(acc_c, h, 0), block_of(back_c, h, 0), bs, br, n_all + 2 + i, right)
                 for i, h in enumerate(back_pieces)]
    col_left = [remote(block_of(acc_c, h, half), block_of(back_c, h, half), bs, br, 2 * n_all + 2 + i, left)
                for i, h in enumerate(back_pieces)]

    def prepare():
        for copy in fetch[1:]:
            copy.wait()
        ramp_i = lax.broadcasted_iota(jnp.int32, (side, side), 0)
        ramp_j = lax.broadcasted_iota(jnp.int32, (side, side), 1)
        take = jnp.where(ramp_i < half, 2 * ramp_i, 2 * ramp_i + 1 - side)
        left = jnp.where(take == ramp_j, 1.0, 0.0).astype(f32)
        take_t = jnp.where(ramp_j < half, 2 * ramp_j, 2 * ramp_j + 1 - side)
        right = jnp.where(take_t == ramp_i, 1.0, 0.0).astype(f32)
        moved = jnp.dot(left, weights_ref[...], precision=lax.Precision.HIGHEST, preferred_element_type=f32)
        wgt[...] = jnp.dot(moved, right, precision=lax.Precision.HIGHEST, preferred_element_type=f32)

        def place(s, carry):
            down, across = offs_ref[0, s], offs_ref[1, s]
            down = jnp.where(down < 0, down + side, down)
            across = jnp.where(across < 0, across + side, across)
            flag = jnp.where(s < count_ref[0, 0], 1.0, 0.0).astype(f32)
            for part in (0, 1):
                rolled = pltpu.roll(probe_ref[part] * flag, down, 0)
                illum[s, part] = pltpu.roll(rolled, across, 1)
            return carry

        lax.fori_loop(0, cap, place, 0)
        scal_ref[0] = jnp.ones_like(scal_ref[0])
        scal_ref[1] = jnp.ones_like(scal_ref[1])
        first = field[...]
        scal_ref[2, 0:1, :] = lanes(jnp.sum(first * first, axis=(0, 1))[None])

    def lanes(value):
        return value[:, :half] + value[:, half:]

    def crosses(s, h):
        return s not in (0, 1) or s != h

    def row_mask(s, h):
        t = lax.broadcasted_iota(jnp.int32, (half, half), 0)
        return t >= offs_ref[0, s] if h == 0 else t < offs_ref[0, s] + half

    def col_mask(s, j):
        u = lax.broadcasted_iota(jnp.int32, (half, half), 1)
        return u >= offs_ref[1, s] if j == 0 else u < offs_ref[1, s] + half

    def span(h):
        return slice(h * half, (h + 1) * half)

    def stage_in(s, place):
        for h in (0, 1):
            wave = []
            for j in (0, 1):
                at = (span(h), span(j))
                view = []
                for part in (0, 1):
                    inner = field[part, *at]
                    if crosses(s, h):
                        inner = jnp.where(row_mask(s, h), inner, halo_r[part, *at])
                    if crosses(s, j):
                        outer = halo_c[part, *at]
                        if crosses(s, h):
                            outer = jnp.where(row_mask(s, h), outer, halo_x[part, *at])
                        inner = jnp.where(col_mask(s, j), inner, outer)
                    view.append(inner)
                pr, pi = illum[s, 0, *at], illum[s, 1, *at]
                wave.append((pr * view[0] - pi * view[1], pr * view[1] + pi * view[0]))
            rows = pl.ds(place * side + h * half, half)
            for which, sign in ((0, 1.0), (1, -1.0)):
                for part in (0, 1):
                    hi, lo = split(wave[0][part] + sign * wave[1][part])
                    wave_hi[which, part, rows] = hi
                    wave_lo[which, part, rows] = lo

    def whole(ref, *at):
        return jnp.concatenate([ref[*at[:1], j, *at[1:]] for j in (0, 1)], axis=1)

    def across(mats, which, rows):
        hi, lo = whole(wave_hi, which, rows), whole(wave_lo, which, rows)
        fine_mat, rest = whole(mats_ref, mats), whole(mats_ref, mats + 1)
        return dot(jnp.concatenate([hi, lo, hi], axis=1), jnp.concatenate([fine_mat, fine_mat, rest], axis=0))

    def down(mats, s, which):
        hi, lo = whole(spec_hi.at[s], which), whole(spec_lo.at[s], which)
        fine_mat, rest = whole(mats_ref, mats), whole(mats_ref, mats + 1)
        return dot(jnp.concatenate([fine_mat, rest, fine_mat], axis=1), jnp.concatenate([hi, hi, lo], axis=0))

    def keep(s, which, j, part, value):
        hi, lo = split(value)
        spec_hi[s, which, j, span(part)] = hi
        spec_lo[s, which, j, span(part)] = lo

    def forward(pair, base):
        for i, s in enumerate(pair):
            stage_in(s, base + i)
        rows = pl.ds(base * side, len(pair) * side)
        found = [across(4 + 2 * which, which, rows) for which in (0, 1)]
        quad = jnp.zeros((half, half), f32)
        for i, s in enumerate(pair):
            top, low = i * side, i * side + half
            for which, sign in ((0, 1.0), (1, -1.0)):
                for j in (0, 1):
                    both = found[j][top:top + half] + sign * found[j][low:low + half]
                    for part in (0, 1):
                        keep(s, which, j, part, both[:, span(part)])
                freq = down(2 * which, s, which)
                for j in (0, 1):
                    scale = wgt[span(which), span(j)]
                    for part in (0, 1):
                        piece = freq[span(part), span(j)]
                        scaled = piece * scale
                        quad = quad + piece * scaled
                        keep(s, which, j, part, scaled)
        return quad

    def inverse(pair, base):
        for i, s in enumerate(pair):
            even = down(4, s, 0)
            odd_ = down(6, s, 1)
            for h, sign in ((0, 1.0), (1, -1.0)):
                both = even + sign * odd_
                rows = pl.ds((base + i) * side + h * half, half)
                for j in (0, 1):
                    for part in (0, 1):
                        hi, lo = split(both[span(part), span(j)])
                        wave_hi[j, part, rows] = hi
                        wave_lo[j, part, rows] = lo
        rows = pl.ds(base * side, len(pair) * side)
        out = [across(2 * j, j, rows) for j in (0, 1)]
        for i, s in enumerate(pair):
            for h in (0, 1):
                mine = slice(i * side + h * half, i * side + (h + 1) * half)
                for j, sign in ((0, 1.0), (1, -1.0)):
                    at = (span(h), span(j))
                    mixed = out[0][mine] + sign * out[1][mine]
                    hr, hi = mixed[:, :half], mixed[:, half:]
                    pr, pi = illum[s, 0, *at], illum[s, 1, *at]
                    for part, term in ((0, pr * hr + pi * hi), (1, pr * hi - pi * hr)):
                        scatter(s, h, j, part, term)

    def add_to(ref, s, first, part, at, value):
        if s == first:
            ref[part, *at] = value
        else:
            ref[part, *at] += value

    def scatter(s, h, j, part, term):
        at = (span(h), span(j))
        inner = term
        if crosses(s, h):
            inner = jnp.where(row_mask(s, h), term, 0.0)
            outer = term - inner
            if crosses(s, j):
                kept = jnp.where(col_mask(s, j), outer, 0.0)
                add_to(acc_x, s, min(t for t in range(cap) if crosses(t, h) and crosses(t, j)), part, at, outer - kept)
                outer = kept
            add_to(acc_r, s, min(t for t in range(cap) if crosses(t, h)), part, at, outer)
        if crosses(s, j):
            kept = jnp.where(col_mask(s, j), inner, 0.0)
            add_to(acc_c, s, min(t for t in range(cap) if crosses(t, j)), part, at, inner - kept)
            inner = kept
        if s == 0:
            inner = inner + ridge_weight * field[part, *at]
        add_to(acc_o, s, 0, part, at, inner)

    def share(msg, mine, k, count, axis, at, i):
        def send(step, carry):
            remote_to = {axis: lax.rem(mine + step, count)}
            pltpu.make_async_remote_copy(
                src_ref=msg.at[k, mine], dst_ref=msg.at[k, mine], send_sem=as_.at[i, k], recv_sem=ar.at[i, k],
                device_id=remote_to, device_id_type=MESH).start()
            return carry
        msg[k, at] = scal_ref[2]
        lax.fori_loop(1, count, send, 0)

    def shared(msg, k, count, sem, i):
        part = msg.at[k, pl.ds(0, count - 1)]
        pltpu.make_async_copy(part, part, sem.at[i, k]).wait()

    def iteration(k, carry):
        pl.when(k == 0)(prepare)
        gather()
        pairs = [tuple(range(cap))]
        quad = sum(forward(pair, pair[0]) for pair in pairs)
        scal_ref[2, 1:2, :] = jnp.sum(quad, axis=0, keepdims=True) + ridge_weight * scal_ref[2, 0:1, :]
        share(msg1, col, k, n_col, "col", col, 0)
        gather_done()
        for pair in pairs:
            inverse(pair, pair[0])

        for copy in back_near:
            copy.start()
        for copy in back_far:
            pl.when(has_far)(copy.start)
        row_near.start()
        for i, (start, size) in enumerate(back_pieces):
            if i < n_near:
                back_near[i].wait_recv()
            else:
                pl.when(has_far)(back_far[i - n_near].wait_recv)
            acc_c[:, pl.ds(start, size), :] += back_x[:, pl.ds(start, size), :]
            pl.when(has_right)(col_right[i].start)
            pl.when(has_left)(col_left[i].start)
            if i == n_near - 1:
                shared(msg1, k, n_col, ar, 0)
                scal_ref[2] = jnp.sum(msg1[k], axis=0)
                share(msg2, row, k, n_row, "row", row, 1)
                pl.when(has_far)(row_far.start)
        shared(msg2, k, n_row, ar, 1)
        total = jnp.sum(jnp.sum(msg2[k], axis=0), axis=1, keepdims=True)
        norm, product = total[0:1], total[1:2]
        norm_before, alpha_before = scal_ref[0, 0:1, 0:1], scal_ref[1, 0:1, 0:1]
        ratio = jnp.where(k == 0, jnp.zeros_like(norm), norm / norm_before)
        alpha = norm / (product - ratio * norm / alpha_before)
        scal_ref[0] = jnp.broadcast_to(norm, scal_ref.shape[1:])
        scal_ref[1] = jnp.broadcast_to(alpha, scal_ref.shape[1:])
        row_near.wait_recv()
        pl.when(has_far)(row_far.wait_recv)
        for i in range(n_all):
            pl.when(has_left)(col_right[i].wait_recv)
            pl.when(has_right)(col_left[i].wait_recv)
        square = jnp.zeros((1, side), f32)
        going = k + 1 < ITERS
        for i, (start, size) in enumerate(gather_pieces):
            rows = pl.ds(start, size)
            before = field[:, rows, :]
            image = acc_o[:, rows, :] + back_r[:, rows, :] + back_c[:, rows, :]
            direction = before + ratio[None] * d_ref[:, rows, :]
            along = image + ratio[None] * along_ref[:, rows, :]
            d_ref[:, rows, :] = direction
            along_ref[:, rows, :] = along
            x_ref[:, rows, :] += alpha[None] * direction
            left_over = before - alpha[None] * along
            field[:, rows, :] = left_over
            square = square + jnp.sum(left_over * left_over, axis=(0, 1))[None]
            if i > 0:
                send_piece(i - 1, going)
        send_piece(n_all - 1, going)
        scal_ref[2, 0:1, :] = lanes(square)
        for copy in back_near:
            copy.wait_send()
        for copy in back_far:
            pl.when(has_far)(copy.wait_send)
        row_near.wait_send()
        pl.when(has_far)(row_far.wait_send)
        for i in range(n_all):
            pl.when(has_right)(col_right[i].wait_send)
            pl.when(has_left)(col_left[i].wait_send)
        shared(msg1, k, n_col, as_, 0)
        shared(msg2, k, n_row, as_, 1)
        return carry

    for i in range(n_all):
        send_piece(i, True)
    lax.fori_loop(0, ITERS, iteration, 0)
    x_out[...] = x_ref[...]
    r_out[...] = field[...]


def local(n_row, n_col, right_side, probe, detector_weights, offsets, counts):
    side, cap = probe.shape[1], offsets.shape[2]
    half = side // 2
    field = pltpu.VMEM((2, side, side), f32)
    vmem = pl.BlockSpec(memory_space=pltpu.VMEM)
    shape = pltpu.VMEM(right_side.shape, f32)
    return pl.pallas_call(
        functools.partial(kernel, n_row, n_col, cap),
        out_shape=(shape, shape),
        in_specs=[pl.BlockSpec(memory_space=pltpu.HBM)] * 6,
        out_specs=(vmem, vmem),
        scratch_shapes=[
            field, pltpu.VMEM((side, side), f32), pltpu.VMEM((8, 2, side, half), bf16),
            pltpu.SMEM((2, cap), jnp.int32), pltpu.SMEM((1, 1), jnp.int32), pltpu.SemaphoreType.DMA((6,)),
        ] + [field] * 11 + [
            pltpu.VMEM((cap, 2, side, side), f32),
            pltpu.VMEM((cap, 2, 2, side, half), bf16),
            pltpu.VMEM((cap, 2, 2, side, half), bf16),
            pltpu.VMEM((2, 2, cap * side, half), bf16),
            pltpu.VMEM((2, 2, cap * side, half), bf16),
            pltpu.VMEM((side, side), f32),
            field, field, field,
            pltpu.VMEM((3, 2, half), f32),
            pltpu.VMEM((ITERS, n_col, 2, half), f32),
            pltpu.VMEM((ITERS, n_row, 2, half), f32),
            pltpu.SemaphoreType.DMA((23,)), pltpu.SemaphoreType.DMA((23,)),
            pltpu.SemaphoreType.DMA((23,)), pltpu.SemaphoreType.DMA((23,)),
            pltpu.SemaphoreType.DMA((2, ITERS)), pltpu.SemaphoreType.DMA((2, ITERS)),
        ],
        compiler_params=pltpu.CompilerParams(collective_id=0, has_side_effects=True),
    )(right_side, probe, detector_weights, jnp.asarray(tables(side)), offsets[0, 0].T, counts)


def solution(mesh):
    in_specs = (P(None, "row", "col"), P(), P(), P("row", "col", None, None), P("row", "col"))
    out_specs = (P(None, "row", "col"), P(None, "row", "col"))
    body = functools.partial(local, mesh.shape["row"], mesh.shape["col"])
    return jax.shard_map(body, mesh=mesh, in_specs=in_specs, out_specs=out_specs, check_vma=False)
```

```python
import functools
import math

import jax
import jax.numpy as jnp
import numpy as np
from jax import lax
from jax.experimental import pallas as pl
from jax.experimental.pallas import tpu as pltpu
from jax.sharding import PartitionSpec as P

ITERS = 3
ridge_weight = 0.5
MESH = pl.DeviceIdType.MESH
f32 = jnp.float32
bf16 = jnp.bfloat16


def tables(side):
    half = side // 2
    n = np.arange(half)
    found = []
    for odd in (0, 1):
        phase = ((2 * np.arange(half) + odd)[:, None] * n[None, :]) % side
        angle = phase * (-2.0 * math.pi / side)
        re, im = np.cos(angle) / math.sqrt(side), np.sin(angle) / math.sqrt(side)
        found.append(np.block([[re, -im], [im, re]]).astype(np.float32))
    full = found + [mat.T.copy() for mat in found]
    out = []
    for mat in full:
        hi = mat.astype(jnp.bfloat16)
        out += [hi, (mat - hi.astype(np.float32)).astype(jnp.bfloat16)]
    return np.stack([np.stack([mat[:, :half], mat[:, half:]]) for mat in out])


def split(value):
    hi = value.astype(bf16)
    return hi, (value - hi.astype(f32)).astype(bf16)


def dot(left, right):
    return jnp.dot(left, right, preferred_element_type=f32)


def kernel(n_row, n_col, cap, right_hbm, probe_hbm, weights_hbm, mats_hbm, offs_hbm, count_hbm,
           both_out,
           probe_ref, weights_ref, mats_ref, offs_ref, count_ref, loads, field, halo_r, halo_c, halo_x, acc_o, acc_r, acc_c, acc_x, back_r, back_c, back_x,
           illum, spec_hi, spec_lo, duo_hi, duo_lo, wave_hi, wave_lo, gain_hi, gain_lo,
           early_ref, rest_ref, term_ref, wgt, x_ref, d_ref, along_ref,
           scal_ref, msg1, msg2, gs, gr, bs, br, as_, ar):
    side = field.shape[1]
    half = side // 2
    row, col = lax.axis_index("row"), lax.axis_index("col")
    odd = lax.rem(row, 2)
    near = row + 1 - 2 * odd
    far = row - 1 + 2 * odd
    has_far = jnp.logical_and(far >= 0, far < n_row)
    has_left, has_right = col > 0, col < n_col - 1
    h_far = pl.multiple_of(odd * half, half)
    h_near = pl.multiple_of(half - odd * half, half)

    fetch = [pltpu.make_async_copy(src, dst, loads.at[i]) for i, (src, dst) in enumerate((
        (right_hbm, field), (probe_hbm, probe_ref), (weights_hbm, weights_ref),
        (mats_hbm, mats_ref), (offs_hbm, offs_ref), (count_hbm, count_ref)))]
    for copy in fetch:
        copy.start()
    barrier = pltpu.get_barrier_semaphore()

    def far_first(count):
        return sorted(range(1, count), key=lambda step: -min(step, count - step))

    for step in far_first(n_col):
        pl.semaphore_signal(barrier, inc=1, device_id={"col": lax.rem(col + step, n_col)}, device_id_type=MESH)
    for step in far_first(n_row):
        pl.semaphore_signal(barrier, inc=1, device_id={"row": lax.rem(row + step, n_row)}, device_id_type=MESH)

    def clear(*views):
        def act():
            for view in views:
                view[...] = jnp.zeros(view.shape, f32)
        return act

    def band(ref, start):
        return ref.at[:, pl.ds(start, half), :]

    lower, upper = pl.ds(0, half), pl.ds(half, half)
    pl.when(jnp.logical_not(has_far))(clear(
        band(halo_r, h_near), band(halo_x, h_near), band(back_r, h_far), band(back_x, h_far)))
    pl.when(jnp.logical_not(has_left))(clear(halo_c.at[:, :, upper], back_c.at[:, :, lower]))
    pl.when(jnp.logical_not(has_right))(clear(halo_c.at[:, :, lower], back_c.at[:, :, upper]))
    for ref in (x_ref, d_ref, along_ref):
        ref[...] = jnp.zeros_like(ref)
    fetch[0].wait()
    pl.semaphore_wait(barrier, n_row + n_col - 2)

    def remote(src, dst, sems, rsems, i, target):
        return pltpu.make_async_remote_copy(
            src_ref=src, dst_ref=dst, send_sem=sems.at[i], recv_sem=rsems.at[i],
            device_id=target, device_id_type=MESH)

    fine = half // 4
    even_cut = [(i * fine, fine) for i in range(4)]
    late_cut = [(0, 2 * fine), (2 * fine, fine), (3 * fine, fine)]
    early_cut = [(0, fine), (fine, fine), (2 * fine, 2 * fine)]

    def spans(*groups):
        return [(pl.multiple_of(start + at, fine), size) for start, cut in groups for at, size in cut]

    def rows_of(ref, start, count=half):
        return ref.at[:, pl.ds(start, count), :]

    def block_of(ref, piece, col_start):
        return ref.at[:, pl.ds(*piece), pl.ds(col_start, half)]

    n_far = len(even_cut)
    n_near = len(late_cut)
    n_all = n_far + n_near
    gather_pieces = spans((h_far, even_cut), (h_near, late_cut))
    back_pieces = spans((h_near, early_cut), (h_far, even_cut))

    left, right = {"col": col - 1}, {"col": col + 1}
    to_left = [remote(block_of(field, h, 0), block_of(halo_c, h, 0), gs, gr, i, left)
               for i, h in enumerate(gather_pieces)]
    to_right = [remote(block_of(field, h, half), block_of(halo_c, h, half), gs, gr, n_all + i, right)
                for i, h in enumerate(gather_pieces)]
    own_far = remote(rows_of(field, h_far), rows_of(halo_r, h_far), gs, gr, 2 * n_all, {"row": far})
    own_near = remote(rows_of(field, h_near), rows_of(halo_r, h_near), gs, gr, 2 * n_all + 1, {"row": near})
    corner = [remote(rows_of(halo_c, *h), rows_of(halo_x, *h), gs, gr, 2 * n_all + 2 + i,
                     {"row": far if i < n_far else near}) for i, h in enumerate(gather_pieces)]

    def if_far(i, action):
        if i < n_far:
            pl.when(has_far)(action)
        else:
            action()

    def send_piece(i, going):
        pl.when(jnp.logical_and(going, has_left))(to_left[i].start)
        pl.when(jnp.logical_and(going, has_right))(to_right[i].start)
        if i == n_far - 1:
            pl.when(jnp.logical_and(going, has_far))(own_far.start)
        if i == n_all - 1:
            pl.when(going)(own_near.start)

    def advance():
        x_ref[...] += scal_ref[1, 0:1, 0:1][None] * d_ref[...]

    def gather():
        def pass_on(i):
            pl.when(has_right)(to_left[i].wait_recv)
            pl.when(has_left)(to_right[i].wait_recv)
            if_far(i, corner[i].start)

        for i in range(n_far):
            pass_on(i)
        own_near.wait_recv()
        pl.when(has_far)(own_far.wait_recv)
        advance()
        early(range(cap // 2))
        for i in range(n_far, n_all):
            pass_on(i)
        early(range(cap // 2, cap))
        for i in range(n_all):
            if_far(i, corner[i].wait_recv)

    def gather_done():
        for i in range(n_all):
            pl.when(has_left)(to_left[i].wait_send)
            pl.when(has_right)(to_right[i].wait_send)
            if_far(i, corner[i].wait_send)
        pl.when(has_far)(own_far.wait_send)
        own_near.wait_send()

    far_out = spans((h_near, even_cut))
    near_out = spans((h_far, early_cut))
    back_far = [remote(rows_of(acc_x, *h), rows_of(back_x, *h), bs, br, i, {"row": far})
                for i, h in enumerate(far_out)]
    back_near = [remote(rows_of(acc_x, *h), rows_of(back_x, *h), bs, br, n_far + i, {"row": near})
                 for i, h in enumerate(near_out)]
    row_far = [remote(rows_of(acc_r, start, 2 * fine), rows_of(back_r, start, 2 * fine), bs, br, at, {"row": far})
               for at, (start, _) in zip((n_all, 3 * n_all + 2), (far_out[0], far_out[2]))]
    row_near = remote(rows_of(acc_r, h_far), rows_of(back_r, h_far), bs, br, n_all + 1, {"row": near})
    col_right = [remote(block_of(acc_c, h, 0), block_of(back_c, h, 0), bs, br, n_all + 2 + i, right)
                 for i, h in enumerate(back_pieces)]
    col_left = [remote(block_of(acc_c, h, half), block_of(back_c, h, half), bs, br, 2 * n_all + 2 + i, left)
                for i, h in enumerate(back_pieces)]

    def prepare():
        for copy in fetch[1:]:
            copy.wait()
        ramp_i = lax.broadcasted_iota(jnp.int32, (side, side), 0)
        ramp_j = lax.broadcasted_iota(jnp.int32, (side, side), 1)
        take = jnp.where(ramp_i < half, 2 * ramp_i, 2 * ramp_i + 1 - side)
        left = jnp.where(take == ramp_j, 1.0, 0.0).astype(f32)
        take_t = jnp.where(ramp_j < half, 2 * ramp_j, 2 * ramp_j + 1 - side)
        right = jnp.where(take_t == ramp_i, 1.0, 0.0).astype(f32)
        moved = jnp.dot(left, weights_ref[...], precision=lax.Precision.HIGHEST, preferred_element_type=f32)
        wgt[...] = jnp.dot(moved, right, precision=lax.Precision.HIGHEST, preferred_element_type=f32)

        def place(s, carry):
            down, across = offs_ref[0, s], offs_ref[1, s]
            down = jnp.where(down < 0, down + side, down)
            across = jnp.where(across < 0, across + side, across)
            flag = jnp.where(s < count_ref[0, 0], 1.0, 0.0).astype(f32)
            flipped = turned(s, side)
            for part in (0, 1):
                rolled = pltpu.roll(probe_ref[part] * flag, down, 0)
                rolled = pltpu.roll(rolled, across, 1)
                lower, upper = rolled[:, :half], rolled[:, half:]
                illum[s, 0, part] = jnp.where(flipped, upper, lower)
                illum[s, 1, part] = jnp.where(flipped, lower, upper)
            return carry

        lax.fori_loop(0, cap, place, 0)
        scal_ref[0] = jnp.ones_like(scal_ref[0])
        scal_ref[1] = jnp.ones_like(scal_ref[1])
        first = field[...]
        scal_ref[2, 0:1, :] = lanes(jnp.sum(first * first, axis=(0, 1))[None])

    def lanes(value):
        return value[:, :half] + value[:, half:]

    def crosses(s, h):
        return s not in (0, 1) or s != h

    def span(h):
        return slice(h * half, (h + 1) * half)

    def row_mask(s, h):
        t = lax.broadcasted_iota(jnp.int32, (half, half), 0)
        return t >= offs_ref[0, s] if h == 0 else t < offs_ref[0, s] + half

    def turned(s, rows=half):
        return jnp.broadcast_to(offs_ref[1, s], (rows, half)) < 0

    def crossing(s, turn, ref, part, h):
        first, second = ref.at[part, span(h), span(0)], ref.at[part, span(h), span(1)]
        if s in (0, 1):
            return (second if s == turn else first)[...]
        if turn == 0:
            return jnp.where(turned(s), second[...], first[...])
        return jnp.where(turned(s), first[...], second[...])

    def own_columns(s):
        u = lax.broadcasted_iota(jnp.int32, (half, half), 1)
        shift = offs_ref[1, s]
        if s == 0:
            return u < shift + half
        if s == 1:
            return u >= shift
        sign = jnp.where(shift < 0, -1, 1)
        return u * sign >= jnp.where(shift < 0, 1 - half - shift, shift)

    def by_column(s, first, second):
        if s == 0:
            return second, first
        if s == 1:
            return first, second
        return jnp.where(turned(s), second, first), jnp.where(turned(s), first, second)

    def lit(s, turn, rows, view):
        pr, pi = illum[s, turn, 0, rows], illum[s, turn, 1, rows]
        return pr * view[0] - pi * view[1], pr * view[1] + pi * view[0]

    def whole(ref, *at):
        return jnp.concatenate([ref[*at, j] for j in (0, 1)], axis=1)

    def triple(ref, at):
        main, rest = whole(ref, at), whole(ref, at + 1)
        return main, rest

    def across(mats, hi_ref, lo_ref, which):
        hi, lo = whole(hi_ref, which), whole(lo_ref, which)
        main, rest = triple(mats_ref, mats)
        return dot(jnp.concatenate([hi, lo, hi], axis=1), jnp.concatenate([main, main, rest], axis=0))

    def down(mats, hi_ref, lo_ref, *at):
        hi, lo = whole(hi_ref, *at), whole(lo_ref, *at)
        main, rest = triple(mats_ref, mats)
        return dot(jnp.concatenate([main, rest, main], axis=1), jnp.concatenate([hi, hi, lo], axis=0))

    def keep(hi_ref, lo_ref, at, value):
        hi, lo = split(value)
        hi_ref[*at] = hi
        lo_ref[*at] = lo

    def early(slots):
        for s in slots:
            own = own_columns(s)
            for turn in (0, 1):
                wave = []
                for h in (0, 1):
                    view = []
                    for part in (0, 1):
                        value = crossing(s, turn, field, part, h)
                        if crosses(s, h):
                            value = jnp.where(row_mask(s, h), value, crossing(s, turn, halo_r, part, h))
                        if turn == 0:
                            value = jnp.where(own, value, 0.0)
                        view.append(value)
                    wave.append(lit(s, turn, span(h), view))
                for which, sign in ((0, 1.0), (1, -1.0)):
                    for part in (0, 1):
                        keep(spec_hi, spec_lo, (s, which, turn, span(part)), wave[0][part] + sign * wave[1][part])
        for s in slots:
            for which in (0, 1):
                found = down(2 * which, spec_hi, spec_lo, s, which)
                first, second = found[:, :half], found[:, half:]
                early_ref[s, 0, which] = first + second
                early_ref[s, 1, which] = first - second

    def late():
        for s in range(cap):
            own = own_columns(s)
            wave = []
            for h in (0, 1):
                view = []
                for part in (0, 1):
                    value = crossing(s, 0, halo_c, part, h)
                    if crosses(s, h):
                        value = jnp.where(row_mask(s, h), value, crossing(s, 0, halo_x, part, h))
                    view.append(jnp.where(own, 0.0, value))
                wave.append(lit(s, 0, span(h), view))
            for which, sign in ((0, 1.0), (1, -1.0)):
                for part in (0, 1):
                    keep(duo_hi, duo_lo, (0, s // 2, which, s % 2, span(part)), wave[0][part] + sign * wave[1][part])
        for pair in range(cap // 2):
            for which in (0, 1):
                found = down(2 * which, duo_hi, duo_lo, 0, pair, which)
                for i in (0, 1):
                    s = 2 * pair + i
                    rows = pl.ds(s * side + which * half, half)
                    for odd_col in (0, 1):
                        total = early_ref[s, odd_col, which] + found[:, span(i)]
                        for part in (0, 1):
                            keep(wave_hi, wave_lo, (odd_col, part, rows), total[span(part)])
        quad = jnp.zeros((side, half), f32)
        for odd_col in (0, 1):
            found = across(4 + 2 * odd_col, wave_hi, wave_lo, odd_col)
            for s in range(cap):
                rows = slice(s * side, (s + 1) * side)
                scale = wgt[:, span(odd_col)]
                for part in (0, 1):
                    piece = found[rows, span(part)]
                    scaled = piece * scale
                    quad = quad + piece * scaled
                    keep(gain_hi, gain_lo, (odd_col, part, pl.ds(s * side, side)), scaled)
        return jnp.sum(quad, axis=0, keepdims=True)

    def add_to(ref, first, part, at, value):
        if first:
            ref[part, *at] = value
        else:
            ref[part, *at] += value

    def terms(s, turn, h, i, even, odd_row):
        both = even[:, span(i)] + odd_row[:, span(i)] if h == 0 else even[:, span(i)] - odd_row[:, span(i)]
        hr, hi = both[:half], both[half:]
        pr, pi = illum[s, turn, 0, span(h)], illum[s, turn, 1, span(h)]
        return pr * hr + pi * hi, pr * hi - pi * hr

    def inverse_crossing():
        found = [across(2 * odd_col, gain_hi, gain_lo, odd_col) for odd_col in (0, 1)]
        for s in range(cap):
            for which in (0, 1):
                rows = slice(s * side + which * half, s * side + (which + 1) * half)
                first, second = found[0][rows] + found[1][rows], found[0][rows] - found[1][rows]
                rest_ref[s, which] = second
                for part in (0, 1):
                    keep(duo_hi, duo_lo, (1, s // 2, which, s % 2, span(part)), first[:, span(part)])
        for pair in range(cap // 2):
            even = down(4, duo_hi, duo_lo, 1, pair, 0)
            odd_row = down(6, duo_hi, duo_lo, 1, pair, 1)
            for i in (0, 1):
                s = 2 * pair + i
                own = own_columns(s)
                for h in (0, 1):
                    for part, term in enumerate(terms(s, 0, h, i, even, odd_row)):
                        term_ref[s, part, span(h)] = term
                        beyond = jnp.where(own, 0.0, term)
                        inner = beyond
                        if crosses(s, h):
                            inner = jnp.where(row_mask(s, h), beyond, 0.0)
                            spread(acc_x, s, h, part, beyond - inner, True)
                        spread(acc_c, s, h, part, inner, False)

    def spread(ref, s, h, part, value, corner_only):
        def first(j):
            able = [t for t in range(cap) if (t > 1 or t != j) and (crosses(t, h) or not corner_only)]
            return s == min(able)
        if s in (0, 1):
            add_to(ref, first(1 - s), part, (span(h), span(1 - s)), value)
        else:
            near_half = jnp.where(turned(s), 0.0, value)
            add_to(ref, first(0), part, (span(h), span(0)), near_half)
            add_to(ref, first(1), part, (span(h), span(1)), value - near_half)

    def inverse_rest():
        for s in range(cap):
            for which in (0, 1):
                for part in (0, 1):
                    keep(duo_hi, duo_lo, (2, s // 2, which, s % 2, span(part)), rest_ref[s, which, :, span(part)])
        for pair in range(cap // 2):
            even = down(4, duo_hi, duo_lo, 2, pair, 0)
            odd_row = down(6, duo_hi, duo_lo, 2, pair, 1)
            for i in (0, 1):
                s = 2 * pair + i
                own = own_columns(s)
                for h in (0, 1):
                    for part, term in enumerate(terms(s, 1, h, i, even, odd_row)):
                        crossed = jnp.where(own, term_ref[s, part, span(h)], 0.0)
                        for j, value in enumerate(by_column(s, crossed, term)):
                            at = (span(h), span(j))
                            inner = value
                            if crosses(s, h):
                                inner = jnp.where(row_mask(s, h), value, 0.0)
                                add_to(acc_r, s == min(t for t in range(cap) if crosses(t, h)), part, at, value - inner)
                            if s == 0:
                                inner = inner + ridge_weight * field[part, *at]
                            add_to(acc_o, s == 0, part, at, inner)

    def share(msg, mine, k, count, axis, at, i):
        def send(step, carry):
            remote_to = {axis: lax.rem(mine + step, count)}
            pltpu.make_async_remote_copy(
                src_ref=msg.at[k, mine], dst_ref=msg.at[k, mine], send_sem=as_.at[i, k], recv_sem=ar.at[i, k],
                device_id=remote_to, device_id_type=MESH).start()
            return carry
        msg[k, at] = scal_ref[2]
        lax.fori_loop(1, count, send, 0)

    def shared(msg, k, count, sem, i):
        part = msg.at[k, pl.ds(0, count - 1)]
        pltpu.make_async_copy(part, part, sem.at[i, k]).wait()

    def iteration(k, carry):
        pl.when(k == 0)(prepare)
        gather()
        quad = late()
        scal_ref[2, 1:2, :] = quad + ridge_weight * scal_ref[2, 0:1, :]
        share(msg1, col, k, n_col, "col", col, 0)
        gather_done()
        inverse_crossing()
        for copy in back_near:
            copy.start()
        for copy in back_far:
            pl.when(has_far)(copy.start)
        inverse_rest()
        row_near.start()
        pl.when(has_far)(row_far[0].start)
        for i, (start, size) in enumerate(back_pieces):
            if i < n_near:
                back_near[i].wait_recv()
            else:
                pl.when(has_far)(back_far[i - n_near].wait_recv)
            acc_c[:, pl.ds(start, size), :] += back_x[:, pl.ds(start, size), :]
            pl.when(has_right)(col_right[i].start)
            pl.when(has_left)(col_left[i].start)
            if i == n_near - 1:
                shared(msg1, k, n_col, ar, 0)
                scal_ref[2] = jnp.sum(msg1[k], axis=0)
                share(msg2, row, k, n_row, "row", row, 1)
                pl.when(has_far)(row_far[1].start)
        shared(msg2, k, n_row, ar, 1)
        total = jnp.sum(jnp.sum(msg2[k], axis=0), axis=1, keepdims=True)
        norm, product = total[0:1], total[1:2]
        norm_before, alpha_before = scal_ref[0, 0:1, 0:1], scal_ref[1, 0:1, 0:1]
        ratio = jnp.where(k == 0, jnp.zeros_like(norm), norm / norm_before)
        alpha = norm / (product - ratio * norm / alpha_before)
        scal_ref[0] = jnp.broadcast_to(norm, scal_ref.shape[1:])
        scal_ref[1] = jnp.broadcast_to(alpha, scal_ref.shape[1:])
        row_near.wait_recv()
        for copy in row_far:
            pl.when(has_far)(copy.wait_recv)
        for i in range(n_all):
            pl.when(has_left)(col_right[i].wait_recv)
            pl.when(has_right)(col_left[i].wait_recv)
        square = jnp.zeros((1, side), f32)
        going = k + 1 < ITERS
        for i, (start, size) in enumerate(gather_pieces):
            rows = pl.ds(start, size)
            before = field[:, rows, :]
            image = acc_o[:, rows, :] + back_r[:, rows, :] + back_c[:, rows, :]
            direction = before + ratio[None] * d_ref[:, rows, :]
            along = image + ratio[None] * along_ref[:, rows, :]
            d_ref[:, rows, :] = direction
            along_ref[:, rows, :] = along
            left_over = before - alpha[None] * along
            field[:, rows, :] = left_over
            square = square + jnp.sum(left_over * left_over, axis=(0, 1))[None]
            if i > 0:
                send_piece(i - 1, going)
        send_piece(n_all - 1, going)
        scal_ref[2, 0:1, :] = lanes(square)
        for copy in back_near:
            copy.wait_send()
        for copy in back_far:
            pl.when(has_far)(copy.wait_send)
        row_near.wait_send()
        for copy in row_far:
            pl.when(has_far)(copy.wait_send)
        for i in range(n_all):
            pl.when(has_right)(col_right[i].wait_send)
            pl.when(has_left)(col_left[i].wait_send)
        shared(msg1, k, n_col, as_, 0)
        shared(msg2, k, n_row, as_, 1)
        return carry

    for i in range(n_all):
        send_piece(i, True)
    lax.fori_loop(0, ITERS, iteration, 0)
    both_out[0] = x_ref[...] + scal_ref[1, 0:1, 0:1][None] * d_ref[...]
    both_out[1] = field[...]


def local(n_row, n_col, right_side, probe, detector_weights, offsets, counts):
    side, cap = probe.shape[1], offsets.shape[2]
    half = side // 2
    field = pltpu.VMEM((2, side, side), f32)
    vmem = pl.BlockSpec(memory_space=pltpu.VMEM)
    both = pl.pallas_call(
        functools.partial(kernel, n_row, n_col, cap),
        out_shape=pltpu.VMEM((2,) + right_side.shape, f32),
        in_specs=[pl.BlockSpec(memory_space=pltpu.HBM)] * 6,
        out_specs=vmem,
        scratch_shapes=[
            field, pltpu.VMEM((side, side), f32), pltpu.VMEM((8, 2, side, half), bf16),
            pltpu.SMEM((2, cap), jnp.int32), pltpu.SMEM((1, 1), jnp.int32), pltpu.SemaphoreType.DMA((6,)),
        ] + [field] * 11 + [
            pltpu.VMEM((cap, 2, 2, side, half), f32),
            pltpu.VMEM((cap, 2, 2, side, half), bf16),
            pltpu.VMEM((cap, 2, 2, side, half), bf16),
            pltpu.VMEM((3, cap // 2, 2, 2, side, half), bf16),
            pltpu.VMEM((3, cap // 2, 2, 2, side, half), bf16),
            pltpu.VMEM((2, 2, cap * side, half), bf16),
            pltpu.VMEM((2, 2, cap * side, half), bf16),
            pltpu.VMEM((2, 2, cap * side, half), bf16),
            pltpu.VMEM((2, 2, cap * side, half), bf16),
            pltpu.VMEM((cap, 2, 2, side, half), f32),
            pltpu.VMEM((cap, 2, half, side), f32),
            pltpu.VMEM((cap, 2, side, half), f32),
            pltpu.VMEM((side, side), f32),
            field, field, field,
            pltpu.VMEM((3, 2, half), f32),
            pltpu.VMEM((ITERS, n_col, 2, half), f32),
            pltpu.VMEM((ITERS, n_row, 2, half), f32),
            pltpu.SemaphoreType.DMA((24,)), pltpu.SemaphoreType.DMA((24,)),
            pltpu.SemaphoreType.DMA((24,)), pltpu.SemaphoreType.DMA((24,)),
            pltpu.SemaphoreType.DMA((2, ITERS)), pltpu.SemaphoreType.DMA((2, ITERS)),
        ],
        compiler_params=pltpu.CompilerParams(collective_id=0, has_side_effects=True),
    )(right_side, probe, detector_weights, jnp.asarray(tables(side)), offsets[0, 0].T, counts)
    return both[0], both[1]


def solution(mesh):
    in_specs = (P(None, "row", "col"), P(), P(), P("row", "col", None, None), P("row", "col"))
    out_specs = (P(None, "row", "col"), P(None, "row", "col"))
    body = functools.partial(local, mesh.shape["row"], mesh.shape["col"])
    return jax.shard_map(body, mesh=mesh, in_specs=in_specs, out_specs=out_specs, check_vma=False)
```

```python
import functools
import math

import jax
import jax.numpy as jnp
import numpy as np
from jax import lax
from jax.experimental import pallas as pl
from jax.experimental.pallas import tpu as pltpu
from jax.sharding import PartitionSpec as P

ITERS = 3
ridge_weight = 0.5
MESH = pl.DeviceIdType.MESH
f32 = jnp.float32
bf16 = jnp.bfloat16


def tables(side):
    half = side // 2
    n = np.arange(half)
    found = []
    for odd in (0, 1):
        phase = ((2 * np.arange(half) + odd)[:, None] * n[None, :]) % side
        angle = phase * (-2.0 * math.pi / side)
        re, im = np.cos(angle) / math.sqrt(side), np.sin(angle) / math.sqrt(side)
        found.append(np.block([[re, -im], [im, re]]).astype(np.float32))
    full = found + [mat.T.copy() for mat in found]
    out = []
    for mat in full:
        hi = mat.astype(jnp.bfloat16)
        out += [hi, (mat - hi.astype(np.float32)).astype(jnp.bfloat16)]
    return np.stack([np.stack([mat[:, :half], mat[:, half:]]) for mat in out])


def split(value):
    hi = value.astype(bf16)
    return hi, (value - hi.astype(f32)).astype(bf16)


def dot(left, right):
    return jnp.dot(left, right, preferred_element_type=f32)


def kernel(n_row, n_col, cap, right_hbm, probe_hbm, weights_hbm, mats_hbm, offs_hbm, count_hbm,
           both_out,
           probe_ref, weights_ref, mats_ref, offs_ref, count_ref, loads, field, halo_r, halo_c, halo_x, acc_o, acc_r, acc_c, acc_x, back_r, back_c, back_x,
           illum, spec_hi, spec_lo, duo_hi, duo_lo, wave_hi, wave_lo, gain_hi, gain_lo,
           early_ref, rest_ref, term_ref, wgt, x_ref, d_ref, along_ref,
           scal_ref, msg1, msg2, gs, gr, bs, br, as_, ar):
    side = field.shape[1]
    half = side // 2
    row, col = lax.axis_index("row"), lax.axis_index("col")
    odd = lax.rem(row, 2)
    near = row + 1 - 2 * odd
    far = row - 1 + 2 * odd
    has_far = jnp.logical_and(far >= 0, far < n_row)
    has_left, has_right = col > 0, col < n_col - 1
    h_far = pl.multiple_of(odd * half, half)
    h_near = pl.multiple_of(half - odd * half, half)

    fetch = [pltpu.make_async_copy(src, dst, loads.at[i]) for i, (src, dst) in enumerate((
        (right_hbm, field), (probe_hbm, probe_ref), (weights_hbm, weights_ref),
        (mats_hbm, mats_ref), (offs_hbm, offs_ref), (count_hbm, count_ref)))]
    for copy in fetch:
        copy.start()
    barrier = pltpu.get_barrier_semaphore()

    def far_first(count):
        return sorted(range(1, count), key=lambda step: -min(step, count - step))

    for step in far_first(n_col):
        pl.semaphore_signal(barrier, inc=1, device_id={"col": lax.rem(col + step, n_col)}, device_id_type=MESH)
    for step in far_first(n_row):
        pl.semaphore_signal(barrier, inc=1, device_id={"row": lax.rem(row + step, n_row)}, device_id_type=MESH)

    def clear(*views):
        def act():
            for view in views:
                view[...] = jnp.zeros(view.shape, f32)
        return act

    def band(ref, start):
        return ref.at[:, pl.ds(start, half), :]

    lower, upper = pl.ds(0, half), pl.ds(half, half)
    pl.when(jnp.logical_not(has_far))(clear(
        band(halo_r, h_near), band(halo_x, h_near), band(back_r, h_far), band(back_x, h_far)))
    pl.when(jnp.logical_not(has_left))(clear(halo_c.at[:, :, upper], back_c.at[:, :, lower]))
    pl.when(jnp.logical_not(has_right))(clear(halo_c.at[:, :, lower], back_c.at[:, :, upper]))
    for ref in (x_ref, d_ref, along_ref):
        ref[...] = jnp.zeros_like(ref)
    fetch[0].wait()
    pl.semaphore_wait(barrier, n_row + n_col - 2)

    def remote(src, dst, sems, rsems, i, target):
        return pltpu.make_async_remote_copy(
            src_ref=src, dst_ref=dst, send_sem=sems.at[i], recv_sem=rsems.at[i],
            device_id=target, device_id_type=MESH)

    fine = half // 4
    even_cut = [(i * fine, fine) for i in range(4)]
    late_cut = [(0, 2 * fine), (2 * fine, fine), (3 * fine, fine)]
    early_cut = [(0, fine), (fine, fine), (2 * fine, 2 * fine)]

    def spans(*groups):
        return [(pl.multiple_of(start + at, fine), size) for start, cut in groups for at, size in cut]

    def rows_of(ref, start, count=half):
        return ref.at[:, pl.ds(start, count), :]

    def block_of(ref, piece, col_start):
        return ref.at[:, pl.ds(*piece), pl.ds(col_start, half)]

    n_far = len(even_cut)
    n_near = len(late_cut)
    n_all = n_far + n_near
    gather_pieces = spans((h_far, even_cut), (h_near, late_cut))
    back_pieces = spans((h_near, early_cut), (h_far, even_cut))

    left, right = {"col": col - 1}, {"col": col + 1}
    to_left = [remote(block_of(field, h, 0), block_of(halo_c, h, 0), gs, gr, i, left)
               for i, h in enumerate(gather_pieces)]
    to_right = [remote(block_of(field, h, half), block_of(halo_c, h, half), gs, gr, n_all + i, right)
                for i, h in enumerate(gather_pieces)]
    own_far = remote(rows_of(field, h_far), rows_of(halo_r, h_far), gs, gr, 2 * n_all, {"row": far})
    own_near = remote(rows_of(field, h_near), rows_of(halo_r, h_near), gs, gr, 2 * n_all + 1, {"row": near})
    corner = [remote(rows_of(halo_c, *h), rows_of(halo_x, *h), gs, gr, 2 * n_all + 2 + i,
                     {"row": far if i < n_far else near}) for i, h in enumerate(gather_pieces)]

    def if_far(i, action):
        if i < n_far:
            pl.when(has_far)(action)
        else:
            action()

    def send_piece(i, going):
        pl.when(jnp.logical_and(going, has_left))(to_left[i].start)
        pl.when(jnp.logical_and(going, has_right))(to_right[i].start)
        if i == n_far - 1:
            pl.when(jnp.logical_and(going, has_far))(own_far.start)
        if i == n_all - 1:
            pl.when(going)(own_near.start)

    def advance():
        x_ref[...] += scal_ref[1, 0:1, 0:1][None] * d_ref[...]

    def gather():
        def pass_on(i):
            pl.when(has_right)(to_left[i].wait_recv)
            pl.when(has_left)(to_right[i].wait_recv)
            if_far(i, corner[i].start)

        for i in range(n_far):
            pass_on(i)
        own_near.wait_recv()
        pl.when(has_far)(own_far.wait_recv)
        advance()
        early(range(cap // 2))
        for i in range(n_far, n_all):
            pass_on(i)
        early(range(cap // 2, cap))
        for i in range(n_all):
            if_far(i, corner[i].wait_recv)

    def gather_done():
        for i in range(n_all):
            pl.when(has_left)(to_left[i].wait_send)
            pl.when(has_right)(to_right[i].wait_send)
            if_far(i, corner[i].wait_send)
        pl.when(has_far)(own_far.wait_send)
        own_near.wait_send()

    far_out = spans((h_near, even_cut))
    near_out = spans((h_far, early_cut))
    back_far = [remote(rows_of(acc_x, *h), rows_of(back_x, *h), bs, br, i, {"row": far})
                for i, h in enumerate(far_out)]
    back_near = [remote(rows_of(acc_x, *h), rows_of(back_x, *h), bs, br, n_far + i, {"row": near})
                 for i, h in enumerate(near_out)]
    row_far = [remote(rows_of(acc_r, start, 2 * fine), rows_of(back_r, start, 2 * fine), bs, br, at, {"row": far})
               for at, (start, _) in zip((n_all, 3 * n_all + 2), (far_out[0], far_out[2]))]
    row_near = remote(rows_of(acc_r, h_far), rows_of(back_r, h_far), bs, br, n_all + 1, {"row": near})
    col_right = [remote(block_of(acc_c, h, 0), block_of(back_c, h, 0), bs, br, n_all + 2 + i, right)
                 for i, h in enumerate(back_pieces)]
    col_left = [remote(block_of(acc_c, h, half), block_of(back_c, h, half), bs, br, 2 * n_all + 2 + i, left)
                for i, h in enumerate(back_pieces)]

    def prepare():
        for copy in fetch[1:]:
            copy.wait()
        ramp_i = lax.broadcasted_iota(jnp.int32, (side, side), 0)
        ramp_j = lax.broadcasted_iota(jnp.int32, (side, side), 1)
        take = jnp.where(ramp_i < half, 2 * ramp_i, 2 * ramp_i + 1 - side)
        left = jnp.where(take == ramp_j, 1.0, 0.0).astype(f32)
        take_t = jnp.where(ramp_j < half, 2 * ramp_j, 2 * ramp_j + 1 - side)
        right = jnp.where(take_t == ramp_i, 1.0, 0.0).astype(f32)
        moved = jnp.dot(left, weights_ref[...], precision=lax.Precision.HIGHEST, preferred_element_type=f32)
        wgt[...] = jnp.dot(moved, right, precision=lax.Precision.HIGHEST, preferred_element_type=f32)

        def place(s, carry):
            down, across = offs_ref[0, s], offs_ref[1, s]
            down = jnp.where(down < 0, down + side, down)
            across = jnp.where(across < 0, across + side, across)
            flag = jnp.where(s < count_ref[0, 0], 1.0, 0.0).astype(f32)
            flipped = turned(s, side)
            for part in (0, 1):
                rolled = pltpu.roll(probe_ref[part] * flag, down, 0)
                rolled = pltpu.roll(rolled, across, 1)
                lower, upper = rolled[:, :half], rolled[:, half:]
                illum[s, 0, part] = jnp.where(flipped, upper, lower)
                illum[s, 1, part] = jnp.where(flipped, lower, upper)
            return carry

        lax.fori_loop(0, cap, place, 0)
        scal_ref[0] = jnp.ones_like(scal_ref[0])
        scal_ref[1] = jnp.ones_like(scal_ref[1])
        first = field[...]
        scal_ref[2, 0:1, :] = lanes(jnp.sum(first * first, axis=(0, 1))[None])

    def lanes(value):
        return value[:, :half] + value[:, half:]

    def crosses(s, h):
        return s not in (0, 1) or s != h

    def span(h):
        return slice(h * half, (h + 1) * half)

    def row_mask(s, h):
        t = lax.broadcasted_iota(jnp.int32, (half, half), 0)
        return t >= offs_ref[0, s] if h == 0 else t < offs_ref[0, s] + half

    def turned(s, rows=half):
        return jnp.broadcast_to(offs_ref[1, s], (rows, half)) < 0

    def crossing(s, turn, ref, part, h):
        first, second = ref.at[part, span(h), span(0)], ref.at[part, span(h), span(1)]
        if s in (0, 1):
            return (second if s == turn else first)[...]
        if turn == 0:
            return jnp.where(turned(s), second[...], first[...])
        return jnp.where(turned(s), first[...], second[...])

    def own_columns(s):
        u = lax.broadcasted_iota(jnp.int32, (half, half), 1)
        shift = offs_ref[1, s]
        if s == 0:
            return u < shift + half
        if s == 1:
            return u >= shift
        sign = jnp.where(shift < 0, -1, 1)
        return u * sign >= jnp.where(shift < 0, 1 - half - shift, shift)

    def by_column(s, first, second):
        if s == 0:
            return second, first
        if s == 1:
            return first, second
        return jnp.where(turned(s), second, first), jnp.where(turned(s), first, second)

    def lit(s, turn, rows, view):
        pr, pi = illum[s, turn, 0, rows], illum[s, turn, 1, rows]
        return pr * view[0] - pi * view[1], pr * view[1] + pi * view[0]

    def whole(ref, *at):
        return jnp.concatenate([ref[*at, j] for j in (0, 1)], axis=1)

    def triple(ref, at):
        main, rest = whole(ref, at), whole(ref, at + 1)
        return main, rest

    def across(mats, hi_ref, lo_ref, which):
        hi, lo = whole(hi_ref, which), whole(lo_ref, which)
        main, rest = triple(mats_ref, mats)
        return dot(jnp.concatenate([hi, lo, hi], axis=1), jnp.concatenate([main, main, rest], axis=0))

    def down(mats, hi_ref, lo_ref, *at):
        hi, lo = whole(hi_ref, *at), whole(lo_ref, *at)
        main, rest = triple(mats_ref, mats)
        return dot(jnp.concatenate([main, rest, main], axis=1), jnp.concatenate([hi, hi, lo], axis=0))

    def keep(hi_ref, lo_ref, at, value):
        hi, lo = split(value)
        hi_ref[*at] = hi
        lo_ref[*at] = lo

    def early(slots):
        for s in slots:
            own = own_columns(s)
            for turn in (0, 1):
                wave = []
                for h in (0, 1):
                    view = []
                    for part in (0, 1):
                        value = crossing(s, turn, field, part, h)
                        if crosses(s, h):
                            value = jnp.where(row_mask(s, h), value, crossing(s, turn, halo_r, part, h))
                        if turn == 0:
                            value = jnp.where(own, value, 0.0)
                        view.append(value)
                    wave.append(lit(s, turn, span(h), view))
                for which, sign in ((0, 1.0), (1, -1.0)):
                    for part in (0, 1):
                        keep(spec_hi, spec_lo, (s, which, turn, span(part)), wave[0][part] + sign * wave[1][part])
        for s in slots:
            for which in (0, 1):
                found = down(2 * which, spec_hi, spec_lo, s, which)
                first, second = found[:, :half], found[:, half:]
                early_ref[s, 0, which] = first + second
                early_ref[s, 1, which] = first - second

    def late():
        for s in range(cap):
            own = own_columns(s)
            wave = []
            for h in (0, 1):
                view = []
                for part in (0, 1):
                    value = crossing(s, 0, halo_c, part, h)
                    if crosses(s, h):
                        value = jnp.where(row_mask(s, h), value, crossing(s, 0, halo_x, part, h))
                    view.append(jnp.where(own, 0.0, value))
                wave.append(lit(s, 0, span(h), view))
            for which, sign in ((0, 1.0), (1, -1.0)):
                for part in (0, 1):
                    keep(duo_hi, duo_lo, (0, s // 2, which, s % 2, span(part)), wave[0][part] + sign * wave[1][part])
        for pair in range(cap // 2):
            for which in (0, 1):
                found = down(2 * which, duo_hi, duo_lo, 0, pair, which)
                for i in (0, 1):
                    s = 2 * pair + i
                    rows = pl.ds(s * side + which * half, half)
                    for odd_col in (0, 1):
                        total = early_ref[s, odd_col, which] + found[:, span(i)]
                        for part in (0, 1):
                            keep(wave_hi, wave_lo, (odd_col, part, rows), total[span(part)])
        quad = jnp.zeros((side, half), f32)
        for odd_col in (0, 1):
            found = across(4 + 2 * odd_col, wave_hi, wave_lo, odd_col)
            for s in range(cap):
                rows = slice(s * side, (s + 1) * side)
                scale = wgt[:, span(odd_col)]
                for part in (0, 1):
                    piece = found[rows, span(part)]
                    scaled = piece * scale
                    quad = quad + piece * scaled
                    keep(gain_hi, gain_lo, (odd_col, part, pl.ds(s * side, side)), scaled)
        return jnp.sum(quad, axis=0, keepdims=True)

    def add_to(ref, first, part, at, value):
        if first:
            ref[part, *at] = value
        else:
            ref[part, *at] += value

    def terms(s, turn, h, i, even, odd_row):
        both = even[:, span(i)] + odd_row[:, span(i)] if h == 0 else even[:, span(i)] - odd_row[:, span(i)]
        hr, hi = both[:half], both[half:]
        pr, pi = illum[s, turn, 0, span(h)], illum[s, turn, 1, span(h)]
        return pr * hr + pi * hi, pr * hi - pi * hr

    def inverse_crossing():
        found = [across(2 * odd_col, gain_hi, gain_lo, odd_col) for odd_col in (0, 1)]
        for s in range(cap):
            for which in (0, 1):
                rows = slice(s * side + which * half, s * side + (which + 1) * half)
                first, second = found[0][rows] + found[1][rows], found[0][rows] - found[1][rows]
                rest_ref[s, which] = second
                for part in (0, 1):
                    keep(duo_hi, duo_lo, (1, s // 2, which, s % 2, span(part)), first[:, span(part)])
        for pair in range(cap // 2):
            even = down(4, duo_hi, duo_lo, 1, pair, 0)
            odd_row = down(6, duo_hi, duo_lo, 1, pair, 1)
            for i in (0, 1):
                s = 2 * pair + i
                own = own_columns(s)
                for h in (0, 1):
                    for part, term in enumerate(terms(s, 0, h, i, even, odd_row)):
                        term_ref[s, part, span(h)] = term
                        beyond = jnp.where(own, 0.0, term)
                        inner = beyond
                        if crosses(s, h):
                            inner = jnp.where(row_mask(s, h), beyond, 0.0)
                            spread(acc_x, s, h, part, beyond - inner, True)
                        spread(acc_c, s, h, part, inner, False)

    def spread(ref, s, h, part, value, corner_only):
        def first(j):
            able = [t for t in range(cap) if (t > 1 or t != j) and (crosses(t, h) or not corner_only)]
            return s == min(able)
        if s in (0, 1):
            add_to(ref, first(1 - s), part, (span(h), span(1 - s)), value)
        else:
            near_half = jnp.where(turned(s), 0.0, value)
            add_to(ref, first(0), part, (span(h), span(0)), near_half)
            add_to(ref, first(1), part, (span(h), span(1)), value - near_half)

    def inverse_rest():
        for s in range(cap):
            for which in (0, 1):
                for part in (0, 1):
                    keep(duo_hi, duo_lo, (2, s // 2, which, s % 2, span(part)), rest_ref[s, which, :, span(part)])
        for pair in range(cap // 2):
            even = down(4, duo_hi, duo_lo, 2, pair, 0)
            odd_row = down(6, duo_hi, duo_lo, 2, pair, 1)
            for i in (0, 1):
                s = 2 * pair + i
                own = own_columns(s)
                for h in (0, 1):
                    for part, term in enumerate(terms(s, 1, h, i, even, odd_row)):
                        crossed = jnp.where(own, term_ref[s, part, span(h)], 0.0)
                        for j, value in enumerate(by_column(s, crossed, term)):
                            at = (span(h), span(j))
                            inner = value
                            if crosses(s, h):
                                inner = jnp.where(row_mask(s, h), value, 0.0)
                                add_to(acc_r, s == min(t for t in range(cap) if crosses(t, h)), part, at, value - inner)
                            if s == 0:
                                inner = inner + ridge_weight * field[part, *at]
                            add_to(acc_o, s == 0, part, at, inner)

    def share(msg, mine, k, count, axis, at, i):
        def send(step, carry):
            remote_to = {axis: lax.rem(mine + step, count)}
            pltpu.make_async_remote_copy(
                src_ref=msg.at[k, mine], dst_ref=msg.at[k, mine], send_sem=as_.at[i, k], recv_sem=ar.at[i, k],
                device_id=remote_to, device_id_type=MESH).start()
            return carry
        msg[k, at] = scal_ref[2]
        lax.fori_loop(1, count, send, 0)

    def shared(msg, k, count, sem, i):
        part = msg.at[k, pl.ds(0, count - 1)]
        pltpu.make_async_copy(part, part, sem.at[i, k]).wait()

    def iteration(k, carry):
        pl.when(k == 0)(prepare)
        gather()
        quad = late()
        scal_ref[2, 1:2, :] = quad + ridge_weight * scal_ref[2, 0:1, :]
        share(msg1, col, k, n_col, "col", col, 0)
        gather_done()
        inverse_crossing()
        for copy in back_near:
            copy.start()
        for copy in back_far:
            pl.when(has_far)(copy.start)
        inverse_rest()
        row_near.start()
        pl.when(has_far)(row_far[0].start)
        for i, (start, size) in enumerate(back_pieces):
            if i < n_near:
                back_near[i].wait_recv()
            else:
                pl.when(has_far)(back_far[i - n_near].wait_recv)
            acc_c[:, pl.ds(start, size), :] += back_x[:, pl.ds(start, size), :]
            pl.when(has_right)(col_right[i].start)
            pl.when(has_left)(col_left[i].start)
            if i == n_near - 1:
                shared(msg1, k, n_col, ar, 0)
                scal_ref[2] = jnp.sum(msg1[k], axis=0)
                share(msg2, row, k, n_row, "row", row, 1)
                pl.when(has_far)(row_far[1].start)
        shared(msg2, k, n_row, ar, 1)
        total = jnp.sum(jnp.sum(msg2[k], axis=0), axis=1, keepdims=True)
        norm, product = total[0:1], total[1:2]
        norm_before, alpha_before = scal_ref[0, 0:1, 0:1], scal_ref[1, 0:1, 0:1]
        ratio = jnp.where(k == 0, jnp.zeros_like(norm), norm / norm_before)
        alpha = norm / (product - ratio * norm / alpha_before)
        scal_ref[0] = jnp.broadcast_to(norm, scal_ref.shape[1:])
        scal_ref[1] = jnp.broadcast_to(alpha, scal_ref.shape[1:])
        def landed(i):
            pl.when(has_left)(col_right[i].wait_recv)
            pl.when(has_right)(col_left[i].wait_recv)

        row_near.wait_recv()
        for i in range(n_near):
            landed(i)
        square = jnp.zeros((1, side), f32)
        going = k + 1 < ITERS
        for i in (*range(n_far, n_all), *range(n_far)):
            start, size = gather_pieces[i]
            rows = pl.ds(start, size)
            if i == 0:
                for copy in row_far:
                    pl.when(has_far)(copy.wait_recv)
            if i < n_far:
                landed(n_near + i)
            before = field[:, rows, :]
            image = acc_o[:, rows, :] + back_r[:, rows, :] + back_c[:, rows, :]
            direction = before + ratio[None] * d_ref[:, rows, :]
            along = image + ratio[None] * along_ref[:, rows, :]
            d_ref[:, rows, :] = direction
            along_ref[:, rows, :] = along
            left_over = before - alpha[None] * along
            field[:, rows, :] = left_over
            square = square + jnp.sum(left_over * left_over, axis=(0, 1))[None]
            if 0 < i < n_far:
                send_piece(i - 1, going)
        for i in range(n_far - 1, n_all):
            send_piece(i, going)
        scal_ref[2, 0:1, :] = lanes(square)
        for copy in back_near:
            copy.wait_send()
        for copy in back_far:
            pl.when(has_far)(copy.wait_send)
        row_near.wait_send()
        for copy in row_far:
            pl.when(has_far)(copy.wait_send)
        for i in range(n_all):
            pl.when(has_right)(col_right[i].wait_send)
            pl.when(has_left)(col_left[i].wait_send)
        shared(msg1, k, n_col, as_, 0)
        shared(msg2, k, n_row, as_, 1)
        return carry

    for i in range(n_all):
        send_piece(i, True)
    lax.fori_loop(0, ITERS, iteration, 0)
    both_out[0] = x_ref[...] + scal_ref[1, 0:1, 0:1][None] * d_ref[...]
    both_out[1] = field[...]


def local(n_row, n_col, right_side, probe, detector_weights, offsets, counts):
    side, cap = probe.shape[1], offsets.shape[2]
    half = side // 2
    field = pltpu.VMEM((2, side, side), f32)
    vmem = pl.BlockSpec(memory_space=pltpu.VMEM)
    both = pl.pallas_call(
        functools.partial(kernel, n_row, n_col, cap),
        out_shape=pltpu.VMEM((2,) + right_side.shape, f32),
        in_specs=[pl.BlockSpec(memory_space=pltpu.HBM)] * 6,
        out_specs=vmem,
        scratch_shapes=[
            field, pltpu.VMEM((side, side), f32), pltpu.VMEM((8, 2, side, half), bf16),
            pltpu.SMEM((2, cap), jnp.int32), pltpu.SMEM((1, 1), jnp.int32), pltpu.SemaphoreType.DMA((6,)),
        ] + [field] * 11 + [
            pltpu.VMEM((cap, 2, 2, side, half), f32),
            pltpu.VMEM((cap, 2, 2, side, half), bf16),
            pltpu.VMEM((cap, 2, 2, side, half), bf16),
            pltpu.VMEM((3, cap // 2, 2, 2, side, half), bf16),
            pltpu.VMEM((3, cap // 2, 2, 2, side, half), bf16),
            pltpu.VMEM((2, 2, cap * side, half), bf16),
            pltpu.VMEM((2, 2, cap * side, half), bf16),
            pltpu.VMEM((2, 2, cap * side, half), bf16),
            pltpu.VMEM((2, 2, cap * side, half), bf16),
            pltpu.VMEM((cap, 2, 2, side, half), f32),
            pltpu.VMEM((cap, 2, half, side), f32),
            pltpu.VMEM((cap, 2, side, half), f32),
            pltpu.VMEM((side, side), f32),
            field, field, field,
            pltpu.VMEM((3, 2, half), f32),
            pltpu.VMEM((ITERS, n_col, 2, half), f32),
            pltpu.VMEM((ITERS, n_row, 2, half), f32),
            pltpu.SemaphoreType.DMA((24,)), pltpu.SemaphoreType.DMA((24,)),
            pltpu.SemaphoreType.DMA((24,)), pltpu.SemaphoreType.DMA((24,)),
            pltpu.SemaphoreType.DMA((2, ITERS)), pltpu.SemaphoreType.DMA((2, ITERS)),
        ],
        compiler_params=pltpu.CompilerParams(collective_id=0, has_side_effects=True),
    )(right_side, probe, detector_weights, jnp.asarray(tables(side)), offsets[0, 0].T, counts)
    return both[0], both[1]


def solution(mesh):
    in_specs = (P(None, "row", "col"), P(), P(), P("row", "col", None, None), P("row", "col"))
    out_specs = (P(None, "row", "col"), P(None, "row", "col"))
    body = functools.partial(local, mesh.shape["row"], mesh.shape["col"])
    return jax.shard_map(body, mesh=mesh, in_specs=in_specs, out_specs=out_specs, check_vma=False)
```
